256 devices in a mesh: member: 4 (over y), lat: 64 (over x, z, core).
Axes of the slice: x: 4, y: 4, z: 8, core: 2. Of those that a mesh axis runs over, the one named last changes fastest.
Arguments:
- ensemble_starting_fields: bfloat16 [4, 256, 512, 384], P('member', 'lat'), may hold values from -6 to 6
- observed: bfloat16 [256, 512, 384], P('lat'), may hold values from -6 to 6
- wave_of_slot: int32 [256], replicated, may hold values from 0 to 255, each once
- leg_forward: bfloat16 [256, 256, 256], P('lat'), may hold values from -0.375 to 0.375
- leg_inverse: bfloat16 [256, 256, 256], P('lat'), may hold values from -0.375 to 0.375
- spec_filter: float32 [2, 256, 384], replicated, may hold values from -5 to 5
- gain_first: float32 [384], replicated, may hold values from 0.5 to 1.5
- gain_second: float32 [384], replicated, may hold values from 0.5 to 1.5
- weight_in: bfloat16 [384, 768], replicated, may hold values from -0.3125 to 0.3125
- weight_out: bfloat16 [768, 384], replicated, may hold values from -0.21875 to 0.21875
Outputs:
- predicted_field: bfloat16 [4, 256, 512, 384], P('member', 'lat')
- proper_loss_slope: bfloat16 [4, 256, 512, 384], P('member', 'lat')
The draws below stay inside these ranges and needn't reach their ends.
Inputs may be any that keep to these rules, and one draw needn't show every extreme that they name: `wave_of_slot`: every wavenumber 0 to 255 sits in exactly one slot.
All inputs are finite; a program needn't handle non-finite values.
Results may differ from the reference program's by a relative error of at most 0.013.
Values may be sent and summed in bfloat16 or wider, within the bound.
A program may use at most 64 MiB of HBM per device.

```python
import jax
import jax.numpy as jnp
from jax import lax

NLAT = 256
NLON = 512
L = 256
M = 256
C = 384
FFN = 768
MEMBERS = 4


def shard_levels(rng, shape, shards, least, high):
    level = 1.0
    for dim, shards_of in shards:
        draws = jax.random.uniform(jax.random.fold_in(jax.random.fold_in(rng, 6), dim), (shards_of,), jnp.float32, least / len(shards), high / len(shards))
        level = level * jnp.repeat(jnp.exp(draws), shape[dim] // shards_of).reshape((-1,) + (1,) * (len(shape) - 1 - dim))
    return level


def scatter_about(key, shape, scale, bound, pieces=(), kind=jnp.bfloat16):
    drawn = scale * jax.random.normal(key, shape, jnp.float32)
    if pieces:
        drawn = drawn * shard_levels(key, shape, pieces, -0.22, 0.18)
    return jnp.clip(drawn, -bound, bound).astype(kind)


def setup_inputs(seed: int = 0) -> dict:
    key_list = jax.random.split(jax.random.key(seed), 11)
    return {
        "ensemble_starting_fields": scatter_about(key_list[0], (MEMBERS, NLAT, NLON, C), 1.0, 6.0, ((0, 4), (1, 64))),
        "observed": scatter_about(key_list[1], (NLAT, NLON, C), 1.0, 6.0, ((0, 64),)),
        "wave_of_slot": jax.random.permutation(key_list[2], M).astype(jnp.int32),
        "leg_forward": scatter_about(key_list[3], (M, L, NLAT), NLAT ** -0.5, 0.375, ((0, 64),)),
        "leg_inverse": scatter_about(key_list[4], (M, NLAT, L), L ** -0.5, 0.375, ((0, 64),)),
        "spec_filter": scatter_about(key_list[5], (2, L, C), 1.0, 5.0, (), jnp.float32),
        "gain_first": jnp.clip(1.0 + 0.1 * jax.random.normal(key_list[6], (C,), jnp.float32), 0.5, 1.5),
        "gain_second": jnp.clip(1.0 + 0.1 * jax.random.normal(key_list[7], (C,), jnp.float32), 0.5, 1.5),
        "weight_in": scatter_about(key_list[8], (C, FFN), C ** -0.5, 0.3125),
        "weight_out": scatter_about(key_list[9], (FFN, C), FFN ** -0.5, 0.21875),
    }


EPS_NORM = 1e-05
EPS_DIST = 1e-06

def layer_norm(values, scales):
    average = lax.optimization_barrier(jnp.mean(values, -1, keepdims=True))
    centred = values - average
    spread = lax.optimization_barrier(jnp.mean(centred * centred, -1, keepdims=True))
    return centred * lax.rsqrt(spread + EPS_NORM) * scales

def distance(first, second):
    return jnp.sqrt(lax.optimization_barrier(jnp.mean(jnp.square(first - second), -1, keepdims=True)) + EPS_DIST)

def reference(ensemble_starting_fields, observed, wave_of_slot, leg_forward, leg_inverse, spec_filter, gain_first, gain_second, weight_in, weight_out):
    order = jnp.arange(L, dtype=jnp.int32)
    retain = (order[None, :] >= wave_of_slot[:, None]).astype(jnp.float32)[:, None, :, None]
    nonzero = (wave_of_slot != 0).astype(jnp.float32)
    table_fwd = leg_forward.astype(jnp.float32)
    table_inv = leg_inverse.astype(jnp.float32)

    def ensemble_increment(state):
        values = state.astype(jnp.float32)
        normed = layer_norm(values, gain_first).astype(jnp.bfloat16)
        spectrum = jnp.fft.rfft(normed.astype(jnp.float32), axis=1) / NLON
        picked = spectrum[:, wave_of_slot, :]
        analysis = jnp.stack([jnp.real(picked), jnp.imag(picked)], 0).astype(jnp.bfloat16)
        coeffs = jnp.einsum('sln,rnsc->srlc', table_fwd, analysis.astype(jnp.float32)) * retain
        real_part = coeffs[:, 0]
        imag_part = coeffs[:, 1]
        filt_real = spec_filter[0]
        filt_imag = spec_filter[1]
        filtered = jnp.stack([real_part * filt_real - imag_part * filt_imag, real_part * filt_imag + imag_part * filt_real], 1).astype(jnp.bfloat16)
        synthesis = jnp.einsum('snl,srlc->srnc', table_inv, filtered.astype(jnp.float32)).astype(jnp.bfloat16)
        synth_real = jnp.transpose(synthesis[:, 0].astype(jnp.float32), (1, 0, 2))
        synth_imag = jnp.transpose(synthesis[:, 1].astype(jnp.float32), (1, 0, 2)) * nonzero[None, :, None]
        blank = jnp.zeros((NLAT, NLON // 2 + 1, C), jnp.float32)
        spectra_full = lax.complex(blank, blank)
        spectra_full = spectra_full.at[:, wave_of_slot, :].set(lax.complex(synth_real, synth_imag))
        spectral = jnp.fft.irfft(spectra_full, n=NLON, axis=1) * NLON
        harmonic_damped_field = values + spectral
        normed_two = layer_norm(harmonic_damped_field, gain_second).astype(jnp.bfloat16).reshape(NLAT * NLON, C)
        hidden = jax.nn.gelu(jnp.dot(normed_two.astype(jnp.float32), weight_in.astype(jnp.float32), preferred_element_type=jnp.float32)).astype(jnp.bfloat16)
        feedforward_result = jnp.dot(hidden.astype(jnp.float32), weight_out.astype(jnp.float32), preferred_element_type=jnp.float32)
        return (harmonic_damped_field + feedforward_result.reshape(NLAT, NLON, C)).astype(jnp.bfloat16)
    predicted_field = lax.map(ensemble_increment, ensemble_starting_fields)

    def score_row(operands):
        rows, target_row = operands
        ensemble = rows.astype(jnp.float32)
        target = target_row.astype(jnp.float32)
        members = ensemble.shape[0]
        grads = []
        for member_index in range(members):
            own = ensemble[member_index]
            pulled = jnp.zeros_like(own)
            for other in range(members):
                pulled = pulled + (own - ensemble[other]) / distance(own, ensemble[other])
            grads.append((own - target) / distance(own, target) - pulled / (members - 1))
        return jnp.stack(grads, 0).astype(jnp.bfloat16)
    latitude_bands = jnp.moveaxis(predicted_field, 1, 0)
    score_rows = lax.map(score_row, (latitude_bands, observed))
    proper_loss_slope = jnp.moveaxis(score_rows, 0, 1)
    return (predicted_field, proper_loss_slope)
```

```python
import functools
import math

import jax
import jax.numpy as jnp
import numpy as np
from jax import lax
from jax.experimental import pallas as pl
from jax.experimental.pallas import tpu as pltpu
from jax.sharding import PartitionSpec as P

EPS_NORM = 1e-05
EPS_DIST = 1e-06
MESH = pl.DeviceIdType.MESH
F32 = jnp.float32
BF16 = jnp.bfloat16


def tables(waves, length):
    m = np.arange(waves)[:, None]
    j = np.arange(length)[None, :]
    angle = (m * j % length) * (2.0 * math.pi / length)
    cosine, sine = np.cos(angle), np.sin(angle)
    forward = np.stack([cosine / length, -sine / length], 1).reshape(2 * waves, length)
    weight = np.where(m == 0, 1.0, 2.0)
    inverse = np.stack([weight * cosine, -weight * sine], 1).reshape(2 * waves, length).T
    return jnp.asarray(forward, BF16), jnp.asarray(inverse, BF16)


def group_order(points, parts):
    rows = np.arange(points * parts)
    part, point = rows // points, rows % points
    order = np.zeros((points * parts, points * parts), np.float32)
    order[rows, point * parts + part] = 1.0
    return jnp.asarray(order, BF16)


def layer_norm(values, scales):
    average = jnp.mean(values, -1, keepdims=True)
    centred = values - average
    spread = jnp.mean(centred * centred, -1, keepdims=True)
    return centred * lax.rsqrt(spread + EPS_NORM) * scales


def inverse_distance(difference):
    return lax.rsqrt(jnp.mean(jnp.square(difference), -1, keepdims=True) + EPS_DIST)


def dot(a, b):
    return jnp.dot(a, b, preferred_element_type=F32)


def kernel(
    x_hbm, obs_hbm, slot_ref, legf_hbm, legi_hbm, filt_hbm, gain1, gain2, win_hbm, wout_hbm,
    cf_hbm, ci_hbm, order_hbm,
    pred_hbm, slope_hbm,
    x, obs, legf, legi, filt, win, wout, cf, ci, order,
    fwd, inv, normed, out_a, in_r, spec, out_b, in_q, pred, in_y, grad, in_z,
    load_sem, x_sem, fs_sem, fr_sem, bs_sem, br_sem, ys_sem, yr_sem, zs_sem, zr_sem, po_sem, so_sem,
):
    members = lax.axis_size("member")
    devices = lax.axis_size("lat")
    me = lax.axis_index("lat")
    mine = lax.axis_index("member")
    rows, length, channels = x.shape
    degrees = legf.shape[1]
    parts = out_a.shape[2]
    slots = parts // 2
    block = length // members
    half = rows // 2
    stride = 27

    def lat_peer(step):
        return (me + stride * step) % devices

    barrier = pltpu.get_barrier_semaphore()

    def greet(step, carry):
        pl.semaphore_signal(barrier, inc=1, device_id=(mine, lat_peer(step)), device_id_type=MESH)
        return carry

    lax.fori_loop(1, devices, greet, 0)
    for step in range(1, members):
        pl.semaphore_signal(
            barrier, inc=1, device_id=((mine + step) % members, me), device_id_type=MESH
        )

    x_loads = [
        pltpu.make_async_copy(x_hbm.at[0, row], x.at[row], x_sem.at[row]) for row in range(rows)
    ]
    sources = [cf_hbm, ci_hbm, order_hbm, legf_hbm, legi_hbm, filt_hbm, win_hbm, wout_hbm]
    places = [cf, ci, order, legf, legi, filt, win, wout]
    loads = [
        pltpu.make_async_copy(source, place, load_sem.at[index])
        for index, (source, place) in enumerate(zip(sources, places))
    ]
    obs_load = pltpu.make_async_copy(
        obs_hbm.at[:, pl.ds(pl.multiple_of(mine * block, block), block), :],
        obs,
        load_sem.at[len(loads)],
    )
    loads[0].start()
    for load in x_loads:
        load.start()
    for load in loads[1:]:
        load.start()
    obs_load.start()

    picks = lax.broadcasted_iota(jnp.int32, (2 * degrees, 2 * degrees), 1)
    picked = jnp.where(slot_ref[...] == picks, 1.0, 0.0).astype(BF16)
    loads[0].wait()
    fwd[...] = dot(picked, cf[...]).astype(BF16)

    def analyse(row):
        def norm_rows(tile, carry):
            at = pl.ds(pl.multiple_of(tile * 128, 128), min(128, length))
            normed[at, :] = layer_norm(x[row, at, :].astype(F32), gain1[...]).astype(BF16)
            return carry

        lax.fori_loop(0, max(length // 128, 1), norm_rows, 0)
        found = dot(fwd[...], normed[...]).astype(BF16)
        out_a[:, row] = found.reshape(devices, parts, channels)

    def send_forward(part):
        def send(step, carry):
            peer = lat_peer(step)
            pltpu.make_async_remote_copy(
                src_ref=out_a.at[peer, pl.ds(part * half, half)],
                dst_ref=in_r.at[me, pl.ds(part * half, half)],
                send_sem=fs_sem.at[part],
                recv_sem=fr_sem.at[part],
                device_id=(mine, peer),
                device_id_type=MESH,
            ).start()
            return carry

        lax.fori_loop(1, devices, send, 0)

    for part in range(2):
        for row in range(part * half, part * half + half):
            x_loads[row].wait()
            analyse(row)
        if part == 0:
            pl.semaphore_wait(barrier, devices - 1 + members - 1)
        send_forward(part)
    in_r[me] = out_a[me]

    loads[1].wait()
    inv[...] = lax.dot_general(
        ci[...], picked, (((1,), (1,)), ((), ())), preferred_element_type=F32
    ).astype(BF16)
    for load in loads[2:]:
        load.wait()
    for slot in range(slots):
        local = slot_ref[pl.ds(pl.multiple_of(me * parts, parts), parts), :][2 * slot : 2 * slot + 1, :]
        level = lax.broadcasted_iota(jnp.int32, (degrees, degrees), 0) * 2
        kept = legf[slot].astype(F32)
        legf[slot] = jnp.where(level >= local, kept, 0.0).astype(BF16)

    for part in range(2):
        everything = in_r.at[pl.ds(0, devices - 1), pl.ds(0, half)]
        pltpu.make_async_copy(everything, everything, fr_sem.at[part]).wait()

    group = order.shape[0] // (rows * parts)
    points = group * rows

    def gather(index, carry):
        taken = in_r[pl.ds(index * group, group)].reshape(points * parts, channels)
        moved = dot(order[...], taken).astype(BF16)
        at = pl.ds(pl.multiple_of(index * points, points), points)
        spec[:, at, :] = moved.reshape(parts, points, channels)
        return carry

    lax.fori_loop(0, devices // group, gather, 0)

    def transform(slot, carry):
        real = dot(legf[slot], spec[2 * slot])
        imag = dot(legf[slot], spec[2 * slot + 1])
        new_real = (real * filt[0] - imag * filt[1]).astype(BF16)
        new_imag = (real * filt[1] + imag * filt[0]).astype(BF16)
        spec[2 * slot] = dot(legi[slot], new_real).astype(BF16)
        spec[2 * slot + 1] = dot(legi[slot], new_imag).astype(BF16)
        return carry

    lax.fori_loop(0, slots, transform, 0)

    def scatter(index, carry):
        at = pl.ds(pl.multiple_of(index * points, points), points)
        taken = spec[:, at, :].reshape(points * parts, channels)
        moved = lax.dot_general(
            order[...], taken, (((0,), (0,)), ((), ())), preferred_element_type=F32
        ).astype(BF16)
        out_b[pl.ds(index * group, group)] = moved.reshape(group, rows, parts, channels)
        return carry

    lax.fori_loop(0, devices // group, scatter, 0)

    def send_back(row, carry):
        def send(step, inner):
            peer = lat_peer(step)
            pltpu.make_async_remote_copy(
                src_ref=out_b.at[peer, row],
                dst_ref=in_q.at[row, me],
                send_sem=bs_sem.at[row],
                recv_sem=br_sem.at[row],
                device_id=(mine, peer),
                device_id_type=MESH,
            ).start()
            return inner

        lax.fori_loop(1, devices, send, 0)
        in_q[row, me] = out_b[me, row]
        return carry

    lax.fori_loop(0, rows, send_back, 0)
    obs_load.wait()

    tall = min(256, length)

    def member_copies(row, source, place, send_sem, recv_sem):
        copies = []
        for step in range(1, members):
            peer = (mine + step) % members
            copies.append(
                pltpu.make_async_remote_copy(
                    src_ref=source(row, peer),
                    dst_ref=place.at[row, mine],
                    send_sem=send_sem.at[row],
                    recv_sem=recv_sem.at[row],
                    device_id=(peer, me),
                    device_id_type=MESH,
                )
            )
        return copies

    def predict(row):
        arrived = in_q.at[row, pl.ds(0, devices - 1)]
        pltpu.make_async_copy(arrived, arrived, br_sem.at[row]).wait()

        def predict_rows(tile, carry):
            at = pl.ds(pl.multiple_of(tile * tall, tall), tall)
            waves = in_q[row].reshape(devices * parts, channels)
            after = x[row, at, :].astype(F32) + dot(inv[at, :], waves)
            second = layer_norm(after, gain2[...]).astype(BF16)
            hidden = jax.nn.gelu(dot(second, win[...])).astype(BF16)
            pred[row, at, :] = (after + dot(hidden, wout[...])).astype(BF16)
            return carry

        lax.fori_loop(0, length // tall, predict_rows, 0)
        at_peer = lambda index, peer: pred.at[
            index, pl.ds(pl.multiple_of(peer * block, block), block), :
        ]
        for copy in member_copies(row, at_peer, in_y, ys_sem, yr_sem):
            copy.start()
        pltpu.make_async_copy(pred.at[row], pred_hbm.at[0, row], po_sem.at[row]).start()

    thin = min(32, block)

    def score(row):
        arrived = in_y.at[row, pl.ds(0, members - 1)]
        pltpu.make_async_copy(arrived, arrived, yr_sem.at[row]).wait()
        in_y[row, mine] = pred[row, pl.ds(pl.multiple_of(mine * block, block), block), :]

        def score_rows(tile, carry):
            at = pl.ds(pl.multiple_of(tile * thin, thin), thin)
            fields = [in_y[row, index, at, :].astype(F32) for index in range(members)]
            target = obs[row, at, :].astype(F32)
            slopes = []
            for index in range(members):
                gap = fields[index] - target
                slopes.append(gap * inverse_distance(gap))
            for first in range(members):
                for second in range(first + 1, members):
                    gap = fields[first] - fields[second]
                    pull = gap * (inverse_distance(gap) * (1.0 / (members - 1)))
                    slopes[first] = slopes[first] - pull
                    slopes[second] = slopes[second] + pull
            for index in range(members):
                grad[row, index, at, :] = slopes[index].astype(BF16)
            return carry

        lax.fori_loop(0, block // thin, score_rows, 0)
        for copy in member_copies(row, lambda index, peer: grad.at[index, peer], in_z, zs_sem, zr_sem):
            copy.start()
        in_z[row, mine] = grad[row, mine]

    def finish(row, carry):
        predict(row)

        @pl.when(row > 0)
        def _():
            score(row - 1)

        return carry

    lax.fori_loop(0, rows, finish, 0)
    score(rows - 1)

    def deliver(row, carry):
        arrived = in_z.at[row, pl.ds(0, members - 1)]
        pltpu.make_async_copy(arrived, arrived, zr_sem.at[row]).wait()
        pltpu.make_async_copy(in_z.at[row], slope_hbm.at[0, row], so_sem.at[row]).start()
        return carry

    lax.fori_loop(0, rows, deliver, 0)

    for part in range(2):
        sent = out_a.at[pl.ds(0, devices - 1), pl.ds(0, half)]
        pltpu.make_async_copy(sent, sent, fs_sem.at[part]).wait()

    def drain(row, carry):
        sent = in_q.at[row, pl.ds(0, devices - 1)]
        pltpu.make_async_copy(sent, sent, bs_sem.at[row]).wait()
        sent = in_y.at[row, pl.ds(0, members - 1)]
        pltpu.make_async_copy(sent, sent, ys_sem.at[row]).wait()
        pltpu.make_async_copy(sent, sent, zs_sem.at[row]).wait()
        pltpu.make_async_copy(pred.at[row], pred_hbm.at[0, row], po_sem.at[row]).wait()
        pltpu.make_async_copy(in_z.at[row], slope_hbm.at[0, row], so_sem.at[row]).wait()
        return carry

    lax.fori_loop(0, rows, drain, 0)


def local(
    ensemble_starting_fields, observed, wave_of_slot, leg_forward, leg_inverse, spec_filter,
    gain_first, gain_second, weight_in, weight_out,
):
    _, rows, length, channels = ensemble_starting_fields.shape
    waves = wave_of_slot.shape[0]
    slots, degrees, lats = leg_forward.shape
    hidden = weight_in.shape[1]
    devices = lax.axis_size("lat")
    members = lax.axis_size("member")
    block = length // members
    parts = 2 * slots
    forward, inverse = tables(waves, length)
    group = min(8, devices)
    order = group_order(group * rows, parts)
    picks = (2 * wave_of_slot[:, None] + jnp.arange(2, dtype=jnp.int32)[None, :]).reshape(-1, 1)
    whole = pl.BlockSpec(memory_space=pl.ANY)
    near = pl.BlockSpec(memory_space=pltpu.VMEM)
    shape = jax.ShapeDtypeStruct((1, rows, length, channels), BF16)
    sems = pltpu.SemaphoreType.DMA
    pred, slope = pl.pallas_call(
        kernel,
        out_shape=(shape, jax.ShapeDtypeStruct((1, rows, members, block, channels), BF16)),
        in_specs=[whole, whole, near, whole, whole, whole, near, near] + [whole] * 5,
        out_specs=(whole, whole),
        scratch_shapes=[
            pltpu.VMEM((rows, length, channels), BF16),
            pltpu.VMEM((rows, block, channels), BF16),
            pltpu.VMEM((slots, degrees, lats), BF16),
            pltpu.VMEM((slots, lats, degrees), BF16),
            pltpu.VMEM((2, degrees, channels), F32),
            pltpu.VMEM((channels, hidden), BF16),
            pltpu.VMEM((hidden, channels), BF16),
            pltpu.VMEM((2 * waves, length), BF16),
            pltpu.VMEM((length, 2 * waves), BF16),
            pltpu.VMEM(order.shape, BF16),
            pltpu.VMEM((2 * waves, length), BF16),
            pltpu.VMEM((length, 2 * waves), BF16),
            pltpu.VMEM((length, channels), BF16),
            pltpu.VMEM((devices, rows, parts, channels), BF16),
            pltpu.VMEM((devices, rows, parts, channels), BF16),
            pltpu.VMEM((parts, lats, channels), BF16),
            pltpu.VMEM((devices, rows, parts, channels), BF16),
            pltpu.VMEM((rows, devices, parts, channels), BF16),
            pltpu.VMEM((rows, length, channels), BF16),
            pltpu.VMEM((rows, members, block, channels), BF16),
            pltpu.VMEM((rows, members, block, channels), BF16),
            pltpu.VMEM((rows, members, block, channels), BF16),
            sems((9,)),
            sems((rows,)),
            sems((2,)),
            sems((2,)),
            sems((rows,)),
            sems((rows,)),
            sems((rows,)),
            sems((rows,)),
            sems((rows,)),
            sems((rows,)),
            sems((rows,)),
            sems((rows,)),
        ],
        compiler_params=pltpu.CompilerParams(
            collective_id=0, has_side_effects=True, vmem_limit_bytes=60 * 1024 * 1024
        ),
    )(
        ensemble_starting_fields, observed, picks, leg_forward, leg_inverse, spec_filter,
        gain_first[None, :], gain_second[None, :], weight_in, weight_out, forward, inverse, order,
    )
    return (pred, slope.reshape(pred.shape))


def solution(mesh):
    in_specs = (
        P("member", "lat", None, None),
        P("lat", None, None),
        P(),
        P("lat", None, None),
        P("lat", None, None),
        P(),
        P(),
        P(),
        P(),
        P(),
    )
    out_specs = (P("member", "lat", None, None), P("member", "lat", None, None))
    return jax.shard_map(local, mesh=mesh, in_specs=in_specs, out_specs=out_specs, check_vma=False)
```

```python
import functools
import math

import jax
import jax.numpy as jnp
import numpy as np
from jax import lax
from jax.experimental import pallas as pl
from jax.experimental.pallas import tpu as pltpu
from jax.sharding import PartitionSpec as P

EPS_NORM = 1e-05
EPS_DIST = 1e-06
MESH = pl.DeviceIdType.MESH
F32 = jnp.float32
BF16 = jnp.bfloat16


def tables(waves, length):
    m = np.arange(waves)[:, None]
    j = np.arange(length)[None, :]
    angle = (m * j % length) * (2.0 * math.pi / length)
    cosine, sine = np.cos(angle), np.sin(angle)
    forward = np.stack([cosine / length, -sine / length], 1).reshape(2 * waves, length)
    weight = np.where(m == 0, 1.0, 2.0)
    inverse = np.stack([weight * cosine, -weight * sine], 1).reshape(2 * waves, length).T
    return jnp.asarray(forward, BF16), jnp.asarray(inverse, BF16)


def group_order(points, parts):
    rows = np.arange(points * parts)
    part, point = rows // points, rows % points
    order = np.zeros((points * parts, points * parts), np.float32)
    order[rows, point * parts + part] = 1.0
    return jnp.asarray(order, BF16)


def layer_norm(values, scales):
    average = jnp.mean(values, -1, keepdims=True)
    centred = values - average
    spread = jnp.mean(centred * centred, -1, keepdims=True)
    return centred * lax.rsqrt(spread + EPS_NORM) * scales


def inverse_distance(difference):
    return lax.rsqrt(jnp.mean(jnp.square(difference), -1, keepdims=True) + EPS_DIST)


def dot(a, b):
    return jnp.dot(a, b, preferred_element_type=F32)


def kernel(
    x_hbm, obs_hbm, slot_hbm, legf_hbm, legi_hbm, filt_hbm, gain1_hbm, gain2_hbm, win_hbm, wout_hbm,
    cf_hbm, ci_hbm, order_hbm,
    pred, in_z,
    x, obs, legf, legi, filt, win, wout, cf, ci, order,
    fwd, inv, normed, out_a, in_r, spec, out_b, in_q, in_y, grad,
    slot_ref, slot_smem, gain1, gain2,
    load_sem, x_sem, fs_sem, fr_sem, bs_sem, br_sem, ys_sem, yr_sem, zs_sem, zr_sem, small_sem,
):
    members = lax.axis_size("member")
    devices = lax.axis_size("lat")
    me = lax.axis_index("lat")
    mine = lax.axis_index("member")
    rows, length, channels = x.shape
    degrees = legf.shape[1]
    parts = out_a.shape[2]
    slots = parts // 2
    block = length // members
    half = rows // 2
    stride = 1

    def lat_peer(step):
        return (me + stride * step) % devices

    barrier = pltpu.get_barrier_semaphore()

    def greet(step, carry):
        pl.semaphore_signal(barrier, inc=1, device_id=(mine, lat_peer(step)), device_id_type=MESH)
        return carry

    lax.fori_loop(1, devices, greet, 0)
    for step in range(1, members):
        pl.semaphore_signal(
            barrier, inc=1, device_id=((mine + step) % members, me), device_id_type=MESH
        )

    x_loads = [
        pltpu.make_async_copy(x_hbm.at[0, row], x.at[row], x_sem.at[row]) for row in range(rows)
    ]
    sources = [cf_hbm, ci_hbm, order_hbm, legf_hbm, legi_hbm, filt_hbm, win_hbm, wout_hbm]
    places = [cf, ci, order, legf, legi, filt, win, wout]
    loads = [
        pltpu.make_async_copy(source, place, load_sem.at[index])
        for index, (source, place) in enumerate(zip(sources, places))
    ]
    obs_load = pltpu.make_async_copy(
        obs_hbm.at[:, pl.ds(pl.multiple_of(mine * block, block), block), :],
        obs,
        load_sem.at[len(loads)],
    )
    small = [
        pltpu.make_async_copy(source, place, small_sem.at[index])
        for index, (source, place) in enumerate(
            [(slot_hbm, slot_ref), (gain1_hbm, gain1), (gain2_hbm, gain2), (slot_hbm, slot_smem)]
        )
    ]
    for load in small:
        load.start()
    loads[0].start()
    for load in x_loads:
        load.start()
    for load in loads[1:]:
        load.start()
    obs_load.start()

    for load in small:
        load.wait()
    spread = (degrees, 2 * degrees)
    gap = lax.broadcasted_iota(jnp.int32, spread, 1) - 2 * lax.broadcasted_iota(jnp.int32, spread, 0)
    twice = jnp.where((gap == 0) | (gap == 1), 2.0, 0.0).astype(BF16)
    waves = jnp.broadcast_to(slot_ref[...].astype(F32)[None, :], (8, degrees)).astype(BF16)
    columns = dot(waves, twice)[0:1].astype(jnp.int32)
    square = (2 * degrees, 2 * degrees)
    columns = columns + lax.broadcasted_iota(jnp.int32, (1, 2 * degrees), 1) % 2
    picked = jnp.where(lax.broadcasted_iota(jnp.int32, square, 0) == columns, 1.0, 0.0).astype(BF16)
    loads[0].wait()
    fwd[...] = lax.dot_general(
        picked, cf[...], (((0,), (0,)), ((), ())), preferred_element_type=F32
    ).astype(BF16)

    def analyse(row):
        def norm_rows(tile, carry):
            at = pl.ds(pl.multiple_of(tile * 128, 128), min(128, length))
            normed[at, :] = layer_norm(x[row, at, :].astype(F32), gain1[...][None, :]).astype(BF16)
            return carry

        lax.fori_loop(0, max(length // 128, 1), norm_rows, 0)
        found = dot(fwd[...], normed[...]).astype(BF16)
        out_a[:, row] = found.reshape(devices, parts, channels)

    def send_forward(part):
        def send(step, carry):
            peer = lat_peer(step)
            pltpu.make_async_remote_copy(
                src_ref=out_a.at[peer, pl.ds(part * half, half)],
                dst_ref=in_r.at[me, pl.ds(part * half, half)],
                send_sem=fs_sem.at[part],
                recv_sem=fr_sem.at[part],
                device_id=(mine, peer),
                device_id_type=MESH,
            ).start()
            return carry

        lax.fori_loop(1, devices, send, 0)

    for part in range(2):
        for row in range(part * half, part * half + half):
            x_loads[row].wait()
            analyse(row)
        if part == 0:
            pl.semaphore_wait(barrier, devices - 1 + members - 1)
        send_forward(part)
    in_r[me] = out_a[me]

    loads[1].wait()
    inv[...] = dot(ci[...], picked).astype(BF16)
    for load in loads[2:]:
        load.wait()
    for slot in range(slots):
        local = slot_smem[me * slots + slot]
        level = lax.broadcasted_iota(jnp.int32, (degrees, degrees), 0)
        kept = legf[slot].astype(F32)
        legf[slot] = jnp.where(level >= local, kept, 0.0).astype(BF16)

    for part in range(2):
        everything = in_r.at[pl.ds(0, devices - 1), pl.ds(0, half)]
        pltpu.make_async_copy(everything, everything, fr_sem.at[part]).wait()

    group = order.shape[0] // (rows * parts)
    points = group * rows

    def gather(index, carry):
        taken = in_r[pl.ds(index * group, group)].reshape(points * parts, channels)
        moved = dot(order[...], taken).astype(BF16)
        at = pl.ds(pl.multiple_of(index * points, points), points)
        spec[:, at, :] = moved.reshape(parts, points, channels)
        return carry

    lax.fori_loop(0, devices // group, gather, 0)

    def transform(slot, carry):
        real = dot(legf[slot], spec[2 * slot])
        imag = dot(legf[slot], spec[2 * slot + 1])
        new_real = (real * filt[0] - imag * filt[1]).astype(BF16)
        new_imag = (real * filt[1] + imag * filt[0]).astype(BF16)
        spec[2 * slot] = dot(legi[slot], new_real).astype(BF16)
        spec[2 * slot + 1] = dot(legi[slot], new_imag).astype(BF16)
        return carry

    lax.fori_loop(0, slots, transform, 0)

    def scatter(index, carry):
        at = pl.ds(pl.multiple_of(index * points, points), points)
        taken = spec[:, at, :].reshape(points * parts, channels)
        moved = lax.dot_general(
            order[...], taken, (((0,), (0,)), ((), ())), preferred_element_type=F32
        ).astype(BF16)
        out_b[pl.ds(index * group, group)] = moved.reshape(group, rows, parts, channels)
        return carry

    lax.fori_loop(0, devices // group, scatter, 0)

    def send_back(row, carry):
        def send(step, inner):
            peer = lat_peer(step)
            pltpu.make_async_remote_copy(
                src_ref=out_b.at[peer, row],
                dst_ref=in_q.at[row, me],
                send_sem=bs_sem.at[row],
                recv_sem=br_sem.at[row],
                device_id=(mine, peer),
                device_id_type=MESH,
            ).start()
            return inner

        lax.fori_loop(1, devices, send, 0)
        in_q[row, me] = out_b[me, row]
        return carry

    lax.fori_loop(0, rows, send_back, 0)
    obs_load.wait()

    tall = min(256, length)

    def member_copies(row, source, place, send_sem, recv_sem):
        copies = []
        for step in range(1, members):
            peer = (mine + step) % members
            copies.append(
                pltpu.make_async_remote_copy(
                    src_ref=source(row, peer),
                    dst_ref=place.at[row, mine],
                    send_sem=send_sem.at[row],
                    recv_sem=recv_sem.at[row],
                    device_id=(peer, me),
                    device_id_type=MESH,
                )
            )
        return copies

    def predict(row):
        arrived = in_q.at[row, pl.ds(0, devices - 1)]
        pltpu.make_async_copy(arrived, arrived, br_sem.at[row]).wait()

        def predict_rows(tile, carry):
            at = pl.ds(pl.multiple_of(tile * tall, tall), tall)
            waves = in_q[row].reshape(devices * parts, channels)
            after = x[row, at, :].astype(F32) + dot(inv[at, :], waves)
            second = layer_norm(after, gain2[...][None, :]).astype(BF16)
            hidden = jax.nn.gelu(dot(second, win[...])).astype(BF16)
            pred[row, at, :] = (after + dot(hidden, wout[...])).astype(BF16)
            return carry

        lax.fori_loop(0, length // tall, predict_rows, 0)
        at_peer = lambda index, peer: pred.at[
            index, pl.ds(pl.multiple_of(peer * block, block), block), :
        ]
        for copy in member_copies(row, at_peer, in_y, ys_sem, yr_sem):
            copy.start()

    thin = min(32, block)

    def score(row):
        arrived = in_y.at[row, pl.ds(0, members - 1)]
        pltpu.make_async_copy(arrived, arrived, yr_sem.at[row]).wait()
        in_y[row, mine] = pred[row, pl.ds(pl.multiple_of(mine * block, block), block), :]

        def score_rows(tile, carry):
            at = pl.ds(pl.multiple_of(tile * thin, thin), thin)
            fields = [in_y[row, index, at, :].astype(F32) for index in range(members)]
            target = obs[row, at, :].astype(F32)
            slopes = []
            for index in range(members):
                gap = fields[index] - target
                slopes.append(gap * inverse_distance(gap))
            for first in range(members):
                for second in range(first + 1, members):
                    gap = fields[first] - fields[second]
                    pull = gap * (inverse_distance(gap) * (1.0 / (members - 1)))
                    slopes[first] = slopes[first] - pull
                    slopes[second] = slopes[second] + pull
            for index in range(members):
                grad[row, index, at, :] = slopes[index].astype(BF16)
            return carry

        lax.fori_loop(0, block // thin, score_rows, 0)
        for copy in member_copies(row, lambda index, peer: grad.at[index, peer], in_z, zs_sem, zr_sem):
            copy.start()
        in_z[row, mine] = grad[row, mine]

    def finish(row, carry):
        predict(row)

        @pl.when(row > 0)
        def _():
            score(row - 1)

        return carry

    lax.fori_loop(0, rows, finish, 0)
    score(rows - 1)

    def deliver(row, carry):
        arrived = in_z.at[row, pl.ds(0, members - 1)]
        pltpu.make_async_copy(arrived, arrived, zr_sem.at[row]).wait()
        return carry

    lax.fori_loop(0, rows, deliver, 0)

    for part in range(2):
        sent = out_a.at[pl.ds(0, devices - 1), pl.ds(0, half)]
        pltpu.make_async_copy(sent, sent, fs_sem.at[part]).wait()

    def drain(row, carry):
        sent = in_q.at[row, pl.ds(0, devices - 1)]
        pltpu.make_async_copy(sent, sent, bs_sem.at[row]).wait()
        sent = in_y.at[row, pl.ds(0, members - 1)]
        pltpu.make_async_copy(sent, sent, ys_sem.at[row]).wait()
        pltpu.make_async_copy(sent, sent, zs_sem.at[row]).wait()
        return carry

    lax.fori_loop(0, rows, drain, 0)


def store(pred, slope, pred_out, slope_out, sem):
    copies = [
        pltpu.make_async_copy(pred, pred_out.at[0], sem.at[0]),
        pltpu.make_async_copy(slope, slope_out.at[0], sem.at[1]),
    ]
    for copy in copies:
        copy.start()
    for copy in copies:
        copy.wait()


def local(
    ensemble_starting_fields, observed, wave_of_slot, leg_forward, leg_inverse, spec_filter,
    gain_first, gain_second, weight_in, weight_out,
):
    _, rows, length, channels = ensemble_starting_fields.shape
    waves = wave_of_slot.shape[0]
    slots, degrees, lats = leg_forward.shape
    hidden = weight_in.shape[1]
    devices = lax.axis_size("lat")
    members = lax.axis_size("member")
    block = length // members
    parts = 2 * slots
    forward, inverse = tables(waves, length)
    group = min(8, devices)
    order = group_order(group * rows, parts)
    whole = pl.BlockSpec(memory_space=pltpu.HBM)
    near = pl.BlockSpec(memory_space=pltpu.VMEM)
    sems = pltpu.SemaphoreType.DMA
    operands = [
        ensemble_starting_fields, observed, wave_of_slot, leg_forward, leg_inverse, spec_filter,
        gain_first, gain_second, weight_in, weight_out, forward, inverse, order,
    ]
    operands = [pltpu.with_memory_space_constraint(operand, pltpu.HBM) for operand in operands]
    pred, slope = pl.pallas_call(
        kernel,
        out_shape=(
            pltpu.VMEM((rows, length, channels), BF16),
            pltpu.VMEM((rows, members, block, channels), BF16),
        ),
        in_specs=[whole] * 13,
        out_specs=(near, near),
        scratch_shapes=[
            pltpu.VMEM((rows, length, channels), BF16),
            pltpu.VMEM((rows, block, channels), BF16),
            pltpu.VMEM((slots, degrees, lats), BF16),
            pltpu.VMEM((slots, lats, degrees), BF16),
            pltpu.VMEM((2, degrees, channels), F32),
            pltpu.VMEM((channels, hidden), BF16),
            pltpu.VMEM((hidden, channels), BF16),
            pltpu.VMEM((2 * waves, length), BF16),
            pltpu.VMEM((length, 2 * waves), BF16),
            pltpu.VMEM(order.shape, BF16),
            pltpu.VMEM((2 * waves, length), BF16),
            pltpu.VMEM((length, 2 * waves), BF16),
            pltpu.VMEM((length, channels), BF16),
            pltpu.VMEM((devices, rows, parts, channels), BF16),
            pltpu.VMEM((devices, rows, parts, channels), BF16),
            pltpu.VMEM((parts, lats, channels), BF16),
            pltpu.VMEM((devices, rows, parts, channels), BF16),
            pltpu.VMEM((rows, devices, parts, channels), BF16),
            pltpu.VMEM((rows, members, block, channels), BF16),
            pltpu.VMEM((rows, members, block, channels), BF16),
            pltpu.VMEM((waves,), jnp.int32),
            pltpu.SMEM((waves,), jnp.int32),
            pltpu.VMEM((channels,), F32),
            pltpu.VMEM((channels,), F32),
            sems((9,)),
            sems((rows,)),
            sems((2,)),
            sems((2,)),
            sems((rows,)),
            sems((rows,)),
            sems((rows,)),
            sems((rows,)),
            sems((rows,)),
            sems((rows,)),
            sems((4,)),
        ],
        compiler_params=pltpu.CompilerParams(
            collective_id=0, has_side_effects=True, vmem_limit_bytes=48 * 1024 * 1024
        ),
    )(*operands)
    results = [pred, slope.reshape(rows, length, channels)]
    results = [pltpu.with_memory_space_constraint(result, pltpu.VMEM) for result in results]
    shape = jax.ShapeDtypeStruct((1, rows, length, channels), BF16)
    pred, slope = pl.pallas_call(
        store,
        out_shape=(shape, shape),
        in_specs=[near, near],
        out_specs=(whole, whole),
        scratch_shapes=[sems((2,))],
    )(*results)
    return (pred, slope)


def solution(mesh):
    in_specs = (
        P("member", "lat", None, None),
        P("lat", None, None),
        P(),
        P("lat", None, None),
        P("lat", None, None),
        P(),
        P(),
        P(),
        P(),
        P(),
    )
    out_specs = (P("member", "lat", None, None), P("member", "lat", None, None))
    return jax.shard_map(local, mesh=mesh, in_specs=in_specs, out_specs=out_specs, check_vma=False)
```

```python
import functools
import math

import jax
import jax.numpy as jnp
import numpy as np
from jax import lax
from jax.experimental import pallas as pl
from jax.experimental.pallas import tpu as pltpu
from jax.sharding import PartitionSpec as P

EPS_NORM = 1e-05
EPS_DIST = 1e-06
MESH = pl.DeviceIdType.MESH
F32 = jnp.float32
BF16 = jnp.bfloat16


def tables(waves, length):
    m = np.arange(waves)[:, None]
    j = np.arange(length)[None, :]
    angle = (m * j % length) * (2.0 * math.pi / length)
    cosine, sine = np.cos(angle), np.sin(angle)
    forward = np.stack([cosine / length, -sine / length], 1).reshape(2 * waves, length)
    weight = np.where(m == 0, 1.0, 2.0)
    inverse = np.stack([weight * cosine, -weight * sine], 1).reshape(2 * waves, length).T
    return jnp.asarray(forward, BF16), jnp.asarray(inverse, BF16)


def group_order(points, parts):
    rows = np.arange(points * parts)
    part, point = rows // points, rows % points
    order = np.zeros((points * parts, points * parts), np.float32)
    order[rows, point * parts + part] = 1.0
    return jnp.asarray(order, BF16)


def layer_norm(values, scales):
    average = jnp.mean(values, -1, keepdims=True)
    centred = values - average
    spread = jnp.mean(centred * centred, -1, keepdims=True)
    return centred * lax.rsqrt(spread + EPS_NORM) * scales


def inverse_distance(difference):
    return lax.rsqrt(jnp.mean(jnp.square(difference), -1, keepdims=True) + EPS_DIST)


def dot(a, b):
    return jnp.dot(a, b, preferred_element_type=F32)


def kernel(
    x_hbm, obs_hbm, slot_hbm, legf_hbm, legi_hbm, filt_hbm, gain1_hbm, gain2_hbm, win_hbm, wout_hbm,
    cf_hbm, ci_hbm, order_hbm,
    pred, in_z,
    x, obs, legf, legi, filt, win, wout, cf, ci, order,
    fwd, inv, normed, out_a, in_r, spec, out_b, in_q, in_y, grad,
    slot_ref, slot_smem, gain1, gain2,
    load_sem, x_sem, fs_sem, fr_sem, bs_sem, br_sem, ys_sem, yr_sem, zs_sem, zr_sem, small_sem,
):
    members = lax.axis_size("member")
    devices = lax.axis_size("lat")
    me = lax.axis_index("lat")
    mine = lax.axis_index("member")
    rows, length, channels = x.shape
    degrees = legf.shape[1]
    parts = out_a.shape[2]
    slots = parts // 2
    block = length // members
    stride = 1

    def lat_peer(step):
        return (me + stride * step) % devices

    barrier = pltpu.get_barrier_semaphore()

    def greet(step, carry):
        pl.semaphore_signal(barrier, inc=1, device_id=(mine, lat_peer(step)), device_id_type=MESH)
        return carry

    lax.fori_loop(1, devices, greet, 0)
    for step in range(1, members):
        pl.semaphore_signal(
            barrier, inc=1, device_id=((mine + step) % members, me), device_id_type=MESH
        )

    x_loads = [
        pltpu.make_async_copy(x_hbm.at[0, row], x.at[row], x_sem.at[row]) for row in range(rows)
    ]
    sources = [cf_hbm, ci_hbm, order_hbm, legf_hbm, legi_hbm, filt_hbm, win_hbm, wout_hbm]
    places = [cf, ci, order, legf, legi, filt, win, wout]
    loads = [
        pltpu.make_async_copy(source, place, load_sem.at[index])
        for index, (source, place) in enumerate(zip(sources, places))
    ]
    obs_load = pltpu.make_async_copy(
        obs_hbm.at[:, pl.ds(pl.multiple_of(mine * block, block), block), :],
        obs,
        load_sem.at[len(loads)],
    )
    small = [
        pltpu.make_async_copy(source, place, small_sem.at[index])
        for index, (source, place) in enumerate(
            [(slot_hbm, slot_ref), (gain1_hbm, gain1), (gain2_hbm, gain2), (slot_hbm, slot_smem)]
        )
    ]
    for load in small:
        load.start()
    loads[0].start()
    for load in x_loads:
        load.start()
    for load in loads[1:]:
        load.start()
    obs_load.start()

    for load in small:
        load.wait()
    spread = (degrees, 2 * degrees)
    gap = lax.broadcasted_iota(jnp.int32, spread, 1) - 2 * lax.broadcasted_iota(jnp.int32, spread, 0)
    twice = jnp.where((gap == 0) | (gap == 1), 2.0, 0.0).astype(BF16)
    waves = jnp.broadcast_to(slot_ref[...].astype(F32)[None, :], (8, degrees)).astype(BF16)
    columns = dot(waves, twice)[0:1].astype(jnp.int32)
    square = (2 * degrees, 2 * degrees)
    columns = columns + lax.broadcasted_iota(jnp.int32, (1, 2 * degrees), 1) % 2
    picked = jnp.where(lax.broadcasted_iota(jnp.int32, square, 0) == columns, 1.0, 0.0).astype(BF16)
    loads[0].wait()
    fwd[...] = lax.dot_general(
        picked, cf[...], (((0,), (0,)), ((), ())), preferred_element_type=F32
    ).astype(BF16)

    first = 2 * channels // 3 // 128 * 128
    chunks = [(0, first), (first, channels - first)]

    def norm_rows(row, carry):
        def norm_tile(tile, inner):
            at = pl.ds(pl.multiple_of(tile * wide, wide), wide)
            normed[row, at, :] = layer_norm(x[row, at, :].astype(F32), gain1[...][None, :]).astype(BF16)
            return inner

        return lax.fori_loop(0, length // wide, norm_tile, carry)

    wide = min(128, length)
    for row in range(rows):
        x_loads[row].wait()
        norm_rows(row, 0)

    for part, (lane, width) in enumerate(chunks):
        lanes = pl.ds(lane, width)

        def analyse(row, carry):
            found = dot(fwd[...], normed[row, :, lanes]).astype(BF16)
            out_a[:, row, :, lanes] = found.reshape(devices, parts, width)
            return carry

        lax.fori_loop(0, rows, analyse, 0)
        if part == 0:
            pl.semaphore_wait(barrier, devices - 1 + members - 1)

        def send(step, carry):
            peer = lat_peer(step)
            pltpu.make_async_remote_copy(
                src_ref=out_a.at[peer, :, :, lanes],
                dst_ref=in_r.at[me, :, :, lanes],
                send_sem=fs_sem.at[part],
                recv_sem=fr_sem.at[part],
                device_id=(mine, peer),
                device_id_type=MESH,
            ).start()
            return carry

        lax.fori_loop(1, devices, send, 0)
    in_r[me] = out_a[me]

    loads[1].wait()
    inv[...] = dot(ci[...], picked).astype(BF16)
    for load in loads[2:]:
        load.wait()
    for slot in range(slots):
        local = slot_smem[me * slots + slot]
        level = lax.broadcasted_iota(jnp.int32, (degrees, degrees), 0)
        kept = legf[slot].astype(F32)
        legf[slot] = jnp.where(level >= local, kept, 0.0).astype(BF16)

    group = order.shape[0] // (rows * parts)
    points = group * rows

    def send_back(row, lanes):
        def send(step, carry):
            peer = lat_peer(step)
            pltpu.make_async_remote_copy(
                src_ref=out_b.at[peer, row, :, lanes],
                dst_ref=in_q.at[row, me, :, lanes],
                send_sem=bs_sem.at[row],
                recv_sem=br_sem.at[row],
                device_id=(mine, peer),
                device_id_type=MESH,
            ).start()
            return carry

        lax.fori_loop(1, devices, send, 0)

    for part, (lane, width) in enumerate(chunks):
        lanes = pl.ds(lane, width)
        everything = in_r.at[pl.ds(0, devices - 1), :, :, lanes]
        pltpu.make_async_copy(everything, everything, fr_sem.at[part]).wait()

        def gather(index, carry):
            taken = in_r[pl.ds(index * group, group), :, :, lanes].reshape(points * parts, width)
            moved = dot(order[...], taken).astype(BF16)
            at = pl.ds(pl.multiple_of(index * points, points), points)
            spec[:, at, lanes] = moved.reshape(parts, points, width)
            return carry

        lax.fori_loop(0, devices // group, gather, 0)

        def transform(slot, carry):
            real = dot(legf[slot], spec[2 * slot, :, lanes])
            imag = dot(legf[slot], spec[2 * slot + 1, :, lanes])
            filt_real, filt_imag = filt[0, :, lanes], filt[1, :, lanes]
            new_real = (real * filt_real - imag * filt_imag).astype(BF16)
            new_imag = (real * filt_imag + imag * filt_real).astype(BF16)
            spec[2 * slot, :, lanes] = dot(legi[slot], new_real).astype(BF16)
            spec[2 * slot + 1, :, lanes] = dot(legi[slot], new_imag).astype(BF16)
            return carry

        lax.fori_loop(0, slots, transform, 0)

        def scatter(index, carry):
            at = pl.ds(pl.multiple_of(index * points, points), points)
            taken = spec[:, at, lanes].reshape(points * parts, width)
            moved = lax.dot_general(
                order[...], taken, (((0,), (0,)), ((), ())), preferred_element_type=F32
            ).astype(BF16)
            out_b[pl.ds(index * group, group), :, :, lanes] = moved.reshape(group, rows, parts, width)
            return carry

        lax.fori_loop(0, devices // group, scatter, 0)
        send_back(0, lanes)

    everywhere = pl.ds(0, channels)

    def send_rest(row, carry):
        send_back(row, everywhere)
        return carry

    lax.fori_loop(1, rows, send_rest, 0)
    for row in range(rows):
        in_q[row, me] = out_b[me, row]
    obs_load.wait()

    halves = in_y.shape[1]
    piece = block // halves
    thin = min(32, piece)

    def spans(half):
        return [
            pl.ds(pl.multiple_of(index * block + half * piece, piece), piece)
            for index in range(members)
        ]

    def predict(row, half):
        waves = in_q[row].reshape(devices * parts, channels)
        table = jnp.concatenate([inv[at, :] for at in spans(half)], 0)
        before = jnp.concatenate([x[row, at, :] for at in spans(half)], 0)
        after = before.astype(F32) + dot(table, waves)
        second = layer_norm(after, gain2[...][None, :]).astype(BF16)
        hidden = jax.nn.gelu(dot(second, win[...])).astype(BF16)
        result = (after + dot(hidden, wout[...])).astype(BF16)
        for index, at in enumerate(spans(half)):
            pred[row, at, :] = result[index * piece : (index + 1) * piece]
        for step in range(1, members):
            peer = (mine + step) % members
            pltpu.make_async_remote_copy(
                src_ref=pred.at[row, pl.ds(pl.multiple_of(peer * block + half * piece, piece), piece), :],
                dst_ref=in_y.at[row, half, mine],
                send_sem=ys_sem.at[row * halves + half],
                recv_sem=yr_sem.at[row * halves + half],
                device_id=(peer, me),
                device_id_type=MESH,
            ).start()

    def score(row, half):
        arrived = in_y.at[row, half, pl.ds(0, members - 1)]
        pltpu.make_async_copy(arrived, arrived, yr_sem.at[row * halves + half]).wait()
        own = pl.ds(pl.multiple_of(mine * block + half * piece, piece), piece)
        in_y[row, half, mine] = pred[row, own, :]

        def score_rows(tile, carry):
            at = pl.ds(pl.multiple_of(tile * thin, thin), thin)
            fields = [in_y[row, half, index, at, :].astype(F32) for index in range(members)]
            here = pl.ds(pl.multiple_of(half * piece + tile * thin, thin), thin)
            target = obs[row, here, :].astype(F32)
            slopes = []
            for index in range(members):
                gap = fields[index] - target
                slopes.append(gap * inverse_distance(gap))
            for one in range(members):
                for two in range(one + 1, members):
                    gap = fields[one] - fields[two]
                    pull = gap * (inverse_distance(gap) * (1.0 / (members - 1)))
                    slopes[one] = slopes[one] - pull
                    slopes[two] = slopes[two] + pull
            for index in range(members):
                grad[row, half, index, at, :] = slopes[index].astype(BF16)
            return carry

        lax.fori_loop(0, piece // thin, score_rows, 0)
        there = pl.ds(pl.multiple_of(half * piece, piece), piece)
        for step in range(1, members):
            peer = (mine + step) % members
            pltpu.make_async_remote_copy(
                src_ref=grad.at[row, half, peer],
                dst_ref=in_z.at[row, mine, there, :],
                send_sem=zs_sem.at[row * halves + half],
                recv_sem=zr_sem.at[row * halves + half],
                device_id=(peer, me),
                device_id_type=MESH,
            ).start()
        in_z[row, mine, there, :] = grad[row, half, mine]

    def finish(row, carry):
        arrived = in_q.at[row, pl.ds(0, devices - 1)]
        pltpu.make_async_copy(arrived, arrived, br_sem.at[row]).wait()

        def predict_half(half, inner):
            predict(row, half)
            return inner

        def score_half(half, inner):
            score(row, half)
            return inner

        lax.fori_loop(0, halves, predict_half, 0)
        lax.fori_loop(0, halves, score_half, 0)
        return carry

    lax.fori_loop(0, rows, finish, 0)

    def deliver(index, carry):
        arrived = in_y.at[0, 0, pl.ds(0, members - 1)]
        pltpu.make_async_copy(arrived, arrived, zr_sem.at[index]).wait()
        pltpu.make_async_copy(arrived, arrived, ys_sem.at[index]).wait()
        pltpu.make_async_copy(arrived, arrived, zs_sem.at[index]).wait()
        return carry

    lax.fori_loop(0, rows * halves, deliver, 0)

    for part, (lane, width) in enumerate(chunks):
        sent = out_a.at[pl.ds(0, devices - 1), :, :, pl.ds(lane, width)]
        pltpu.make_async_copy(sent, sent, fs_sem.at[part]).wait()

    def drain(row, carry):
        sent = in_q.at[row, pl.ds(0, devices - 1)]
        pltpu.make_async_copy(sent, sent, bs_sem.at[row]).wait()
        return carry

    lax.fori_loop(0, rows, drain, 0)


def store(pred, slope, pred_out, slope_out, sem):
    copies = [
        pltpu.make_async_copy(pred, pred_out.at[0], sem.at[0]),
        pltpu.make_async_copy(slope, slope_out.at[0], sem.at[1]),
    ]
    for copy in copies:
        copy.start()
    for copy in copies:
        copy.wait()


def local(
    ensemble_starting_fields, observed, wave_of_slot, leg_forward, leg_inverse, spec_filter,
    gain_first, gain_second, weight_in, weight_out,
):
    _, rows, length, channels = ensemble_starting_fields.shape
    waves = wave_of_slot.shape[0]
    slots, degrees, lats = leg_forward.shape
    hidden = weight_in.shape[1]
    devices = lax.axis_size("lat")
    members = lax.axis_size("member")
    block = length // members
    parts = 2 * slots
    halves = 2
    forward, inverse = tables(waves, length)
    group = min(8, devices)
    order = group_order(group * rows, parts)
    whole = pl.BlockSpec(memory_space=pltpu.HBM)
    near = pl.BlockSpec(memory_space=pltpu.VMEM)
    sems = pltpu.SemaphoreType.DMA
    operands = [
        ensemble_starting_fields, observed, wave_of_slot, leg_forward, leg_inverse, spec_filter,
        gain_first, gain_second, weight_in, weight_out, forward, inverse, order,
    ]
    operands = [pltpu.with_memory_space_constraint(operand, pltpu.HBM) for operand in operands]
    pred, slope = pl.pallas_call(
        kernel,
        out_shape=(
            pltpu.VMEM((rows, length, channels), BF16),
            pltpu.VMEM((rows, members, block, channels), BF16),
        ),
        in_specs=[whole] * 13,
        out_specs=(near, near),
        scratch_shapes=[
            pltpu.VMEM((rows, length, channels), BF16),
            pltpu.VMEM((rows, block, channels), BF16),
            pltpu.VMEM((slots, degrees, lats), BF16),
            pltpu.VMEM((slots, lats, degrees), BF16),
            pltpu.VMEM((2, degrees, channels), F32),
            pltpu.VMEM((channels, hidden), BF16),
            pltpu.VMEM((hidden, channels), BF16),
            pltpu.VMEM((2 * waves, length), BF16),
            pltpu.VMEM((length, 2 * waves), BF16),
            pltpu.VMEM(order.shape, BF16),
            pltpu.VMEM((2 * waves, length), BF16),
            pltpu.VMEM((length, 2 * waves), BF16),
            pltpu.VMEM((rows, length, channels), BF16),
            pltpu.VMEM((devices, rows, parts, channels), BF16),
            pltpu.VMEM((devices, rows, parts, channels), BF16),
            pltpu.VMEM((parts, lats, channels), BF16),
            pltpu.VMEM((devices, rows, parts, channels), BF16),
            pltpu.VMEM((rows, devices, parts, channels), BF16),
            pltpu.VMEM((rows, halves, members, block // halves, channels), BF16),
            pltpu.VMEM((rows, halves, members, block // halves, channels), BF16),
            pltpu.VMEM((waves,), jnp.int32),
            pltpu.SMEM((waves,), jnp.int32),
            pltpu.VMEM((channels,), F32),
            pltpu.VMEM((channels,), F32),
            sems((9,)),
            sems((rows,)),
            sems((2,)),
            sems((2,)),
            sems((rows,)),
            sems((rows,)),
            sems((rows * halves,)),
            sems((rows * halves,)),
            sems((rows * halves,)),
            sems((rows * halves,)),
            sems((4,)),
        ],
        compiler_params=pltpu.CompilerParams(
            collective_id=0, has_side_effects=True, vmem_limit_bytes=48 * 1024 * 1024
        ),
    )(*operands)
    results = [pred, slope.reshape(rows, length, channels)]
    results = [pltpu.with_memory_space_constraint(result, pltpu.VMEM) for result in results]
    shape = jax.ShapeDtypeStruct((1, rows, length, channels), BF16)
    pred, slope = pl.pallas_call(
        store,
        out_shape=(shape, shape),
        in_specs=[near, near],
        out_specs=(whole, whole),
        scratch_shapes=[sems((2,))],
    )(*results)
    return (pred, slope)


def solution(mesh):
    in_specs = (
        P("member", "lat", None, None),
        P("lat", None, None),
        P(),
        P("lat", None, None),
        P("lat", None, None),
        P(),
        P(),
        P(),
        P(),
        P(),
    )
    out_specs = (P("member", "lat", None, None), P("member", "lat", None, None))
    return jax.shard_map(local, mesh=mesh, in_specs=in_specs, out_specs=out_specs, check_vma=False)
```

```python
import functools
import math

import jax
import jax.numpy as jnp
import numpy as np
from jax import lax
from jax.experimental import pallas as pl
from jax.experimental.pallas import tpu as pltpu
from jax.sharding import PartitionSpec as P

EPS_NORM = 1e-05
EPS_DIST = 1e-06
MESH = pl.DeviceIdType.MESH
F32 = jnp.float32
BF16 = jnp.bfloat16


def tables(waves, length):
    m = np.arange(waves)[:, None]
    j = np.arange(length)[None, :]
    angle = (m * j % length) * (2.0 * math.pi / length)
    cosine, sine = np.cos(angle), np.sin(angle)
    forward = np.stack([cosine / length, -sine / length], 1).reshape(2 * waves, length)
    weight = np.where(m == 0, 1.0, 2.0)
    inverse = np.stack([weight * cosine, -weight * sine], 1).reshape(2 * waves, length).T
    return jnp.asarray(forward, BF16), jnp.asarray(inverse, BF16)


def group_order(points, parts):
    rows = np.arange(points * parts)
    part, point = rows // points, rows % points
    order = np.zeros((points * parts, points * parts), np.float32)
    order[rows, point * parts + part] = 1.0
    return jnp.asarray(order, BF16)


def layer_norm(values, scales):
    average = jnp.mean(values, -1, keepdims=True)
    centred = values - average
    spread = jnp.mean(centred * centred, -1, keepdims=True)
    return centred * lax.rsqrt(spread + EPS_NORM) * scales


def inverse_distance(difference):
    return lax.rsqrt(jnp.mean(jnp.square(difference), -1, keepdims=True) + EPS_DIST)


def dot(a, b):
    return jnp.dot(a, b, preferred_element_type=F32)


def kernel(
    x_hbm, obs_hbm, slot_hbm, legf_hbm, legi_hbm, filt_hbm, gain1_hbm, gain2_hbm, win_hbm, wout_hbm,
    cf_hbm, ci_hbm, order_hbm,
    pred, in_z,
    x, obs, legf, legi, filt, win, wout, cf, ci, order,
    fwd, inv, normed, out_a, in_r, spec, out_b, in_q, in_y, grad,
    slot_ref, slot_smem, gain1, gain2,
    load_sem, x_sem, fs_sem, fr_sem, bs_sem, br_sem, ys_sem, yr_sem, zs_sem, zr_sem, small_sem,
):
    members = lax.axis_size("member")
    devices = lax.axis_size("lat")
    me = lax.axis_index("lat")
    mine = lax.axis_index("member")
    rows, length, channels = x.shape
    degrees = legf.shape[1]
    parts = out_a.shape[2]
    slots = parts // 2
    block = length // members
    stride = 1

    def lat_peer(step):
        return (me + stride * step) % devices

    barrier = pltpu.get_barrier_semaphore()

    def greet(step, carry):
        pl.semaphore_signal(barrier, inc=1, device_id=(mine, lat_peer(step)), device_id_type=MESH)
        return carry

    lax.fori_loop(devices // 2, devices, greet, 0)
    lax.fori_loop(1, devices // 2, greet, 0)
    for step in range(1, members):
        pl.semaphore_signal(
            barrier, inc=1, device_id=((mine + step) % members, me), device_id_type=MESH
        )

    x_loads = [
        pltpu.make_async_copy(x_hbm.at[0, row], x.at[row], x_sem.at[row]) for row in range(rows)
    ]
    sources = [cf_hbm, ci_hbm, order_hbm, legf_hbm, legi_hbm, filt_hbm, win_hbm, wout_hbm]
    places = [cf, ci, order, legf, legi, filt, win, wout]
    loads = [
        pltpu.make_async_copy(source, place, load_sem.at[index])
        for index, (source, place) in enumerate(zip(sources, places))
    ]
    obs_load = pltpu.make_async_copy(
        obs_hbm.at[:, pl.ds(pl.multiple_of(mine * block, block), block), :],
        obs,
        load_sem.at[len(loads)],
    )
    small = [
        pltpu.make_async_copy(source, place, small_sem.at[index])
        for index, (source, place) in enumerate(
            [(slot_hbm, slot_ref), (gain1_hbm, gain1), (gain2_hbm, gain2), (slot_hbm, slot_smem)]
        )
    ]
    for load in small:
        load.start()
    loads[0].start()
    for load in x_loads:
        load.start()
    for load in loads[1:]:
        load.start()
    obs_load.start()

    for load in small:
        load.wait()
    spread = (degrees, 2 * degrees)
    gap = lax.broadcasted_iota(jnp.int32, spread, 1) - 2 * lax.broadcasted_iota(jnp.int32, spread, 0)
    twice = jnp.where((gap == 0) | (gap == 1), 2.0, 0.0).astype(BF16)
    waves = jnp.broadcast_to(slot_ref[...].astype(F32)[None, :], (8, degrees)).astype(BF16)
    columns = dot(waves, twice)[0:1].astype(jnp.int32)
    square = (2 * degrees, 2 * degrees)
    columns = columns + lax.broadcasted_iota(jnp.int32, (1, 2 * degrees), 1) % 2
    picked = jnp.where(lax.broadcasted_iota(jnp.int32, square, 0) == columns, 1.0, 0.0).astype(BF16)
    loads[0].wait()
    fwd[...] = lax.dot_general(
        picked, cf[...], (((0,), (0,)), ((), ())), preferred_element_type=F32
    ).astype(BF16)

    first = 2 * channels // 3 // 128 * 128
    chunks = [(0, first), (first, channels - first)]

    def norm_rows(row, carry):
        def norm_tile(tile, inner):
            at = pl.ds(pl.multiple_of(tile * wide, wide), wide)
            normed[row, at, :] = layer_norm(x[row, at, :].astype(F32), gain1[...][None, :]).astype(BF16)
            return inner

        return lax.fori_loop(0, length // wide, norm_tile, carry)

    wide = min(256, length)

    def analyse_and_send(start, count, part):
        lane, width = chunks[part]
        lanes = pl.ds(lane, width)
        these = pl.ds(start, count)

        def analyse(row, carry):
            found = dot(fwd[...], normed[row, :, lanes]).astype(BF16)
            out_a[:, row, :, lanes] = found.reshape(devices, parts, width)
            return carry

        lax.fori_loop(start, start + count, analyse, 0)
        if start == 0 and part == 0:
            pl.semaphore_wait(barrier, devices - 1 + members - 1)

        def send(step, carry):
            peer = lat_peer(step)
            pltpu.make_async_remote_copy(
                src_ref=out_a.at[peer, these, :, lanes],
                dst_ref=in_r.at[me, these, :, lanes],
                send_sem=fs_sem.at[part],
                recv_sem=fr_sem.at[part],
                device_id=(mine, peer),
                device_id_type=MESH,
            ).start()
            return carry

        lax.fori_loop(1, devices, send, 0)

    pair = rows // 2
    for start in range(0, rows, pair):
        for row in range(start, start + pair):
            x_loads[row].wait()
        lax.fori_loop(start, start + pair, norm_rows, 0)
        analyse_and_send(start, pair, 0)
    analyse_and_send(0, rows, 1)
    in_r[me] = out_a[me]

    loads[1].wait()
    inv[...] = dot(ci[...], picked).astype(BF16)
    for load in loads[2:]:
        load.wait()
    for slot in range(slots):
        local = slot_smem[me * slots + slot]
        level = lax.broadcasted_iota(jnp.int32, (degrees, degrees), 0)
        kept = legf[slot].astype(F32)
        legf[slot] = jnp.where(level >= local, kept, 0.0).astype(BF16)

    group = order.shape[0] // (rows * parts)
    points = group * rows

    def send_back(row, lanes):
        def send(step, carry):
            peer = lat_peer(step)
            pltpu.make_async_remote_copy(
                src_ref=out_b.at[peer, row, :, lanes],
                dst_ref=in_q.at[row, me, :, lanes],
                send_sem=bs_sem.at[row],
                recv_sem=br_sem.at[row],
                device_id=(mine, peer),
                device_id_type=MESH,
            ).start()
            return carry

        lax.fori_loop(1, devices, send, 0)

    for part, (lane, width) in enumerate(chunks):
        lanes = pl.ds(lane, width)
        everything = in_r.at[pl.ds(0, devices - 1), :, :, lanes]
        pltpu.make_async_copy(everything, everything, fr_sem.at[part]).wait()

        def gather(index, carry):
            taken = in_r[pl.ds(index * group, group), :, :, lanes].reshape(points * parts, width)
            moved = dot(order[...], taken).astype(BF16)
            at = pl.ds(pl.multiple_of(index * points, points), points)
            spec[:, at, lanes] = moved.reshape(parts, points, width)
            return carry

        lax.fori_loop(0, devices // group, gather, 0)

        def transform(slot, carry):
            real = dot(legf[slot], spec[2 * slot, :, lanes])
            imag = dot(legf[slot], spec[2 * slot + 1, :, lanes])
            filt_real, filt_imag = filt[0, :, lanes], filt[1, :, lanes]
            new_real = (real * filt_real - imag * filt_imag).astype(BF16)
            new_imag = (real * filt_imag + imag * filt_real).astype(BF16)
            spec[2 * slot, :, lanes] = dot(legi[slot], new_real).astype(BF16)
            spec[2 * slot + 1, :, lanes] = dot(legi[slot], new_imag).astype(BF16)
            return carry

        lax.fori_loop(0, slots, transform, 0)

        def scatter(index, carry):
            at = pl.ds(pl.multiple_of(index * points, points), points)
            taken = spec[:, at, lanes].reshape(points * parts, width)
            moved = lax.dot_general(
                order[...], taken, (((0,), (0,)), ((), ())), preferred_element_type=F32
            ).astype(BF16)
            out_b[pl.ds(index * group, group), :, :, lanes] = moved.reshape(group, rows, parts, width)
            return carry

        lax.fori_loop(0, devices // group, scatter, 0)
        send_back(0, lanes)

    everywhere = pl.ds(0, channels)

    def send_rest(row, carry):
        send_back(row, everywhere)
        return carry

    lax.fori_loop(1, rows, send_rest, 0)
    for row in range(rows):
        in_q[row, me] = out_b[me, row]
    obs_load.wait()

    halves = in_y.shape[1]
    piece = block // halves
    thin = min(32, piece)

    def spans(half):
        return [
            pl.ds(pl.multiple_of(index * block + half * piece, piece), piece)
            for index in range(members)
        ]

    def predict(row, half):
        waves = in_q[row].reshape(devices * parts, channels)
        table = jnp.concatenate([inv[at, :] for at in spans(half)], 0)
        before = jnp.concatenate([x[row, at, :] for at in spans(half)], 0)
        after = before.astype(F32) + dot(table, waves)
        second = layer_norm(after, gain2[...][None, :]).astype(BF16)
        hidden = jax.nn.gelu(dot(second, win[...])).astype(BF16)
        result = (after + dot(hidden, wout[...])).astype(BF16)
        for index, at in enumerate(spans(half)):
            pred[row, at, :] = result[index * piece : (index + 1) * piece]
        for step in range(1, members):
            peer = (mine + step) % members
            pltpu.make_async_remote_copy(
                src_ref=pred.at[row, pl.ds(pl.multiple_of(peer * block + half * piece, piece), piece), :],
                dst_ref=in_y.at[row, half, mine],
                send_sem=ys_sem.at[row * halves + half],
                recv_sem=yr_sem.at[row * halves + half],
                device_id=(peer, me),
                device_id_type=MESH,
            ).start()

    def score(row, half):
        arrived = in_y.at[row, half, pl.ds(0, members - 1)]
        pltpu.make_async_copy(arrived, arrived, yr_sem.at[row * halves + half]).wait()
        own = pl.ds(pl.multiple_of(mine * block + half * piece, piece), piece)
        in_y[row, half, mine] = pred[row, own, :]

        def score_rows(tile, carry):
            at = pl.ds(pl.multiple_of(tile * thin, thin), thin)
            fields = [in_y[row, half, index, at, :].astype(F32) for index in range(members)]
            here = pl.ds(pl.multiple_of(half * piece + tile * thin, thin), thin)
            target = obs[row, here, :].astype(F32)
            slopes = []
            for index in range(members):
                gap = fields[index] - target
                slopes.append(gap * inverse_distance(gap))
            for one in range(members):
                for two in range(one + 1, members):
                    gap = fields[one] - fields[two]
                    pull = gap * (inverse_distance(gap) * (1.0 / (members - 1)))
                    slopes[one] = slopes[one] - pull
                    slopes[two] = slopes[two] + pull
            for index in range(members):
                grad[row, half, index, at, :] = slopes[index].astype(BF16)
            return carry

        lax.fori_loop(0, piece // thin, score_rows, 0)
        there = pl.ds(pl.multiple_of(half * piece, piece), piece)
        for step in range(1, members):
            peer = (mine + step) % members
            pltpu.make_async_remote_copy(
                src_ref=grad.at[row, half, peer],
                dst_ref=in_z.at[row, mine, there, :],
                send_sem=zs_sem.at[row * halves + half],
                recv_sem=zr_sem.at[row * halves + half],
                device_id=(peer, me),
                device_id_type=MESH,
            ).start()
        in_z[row, mine, there, :] = grad[row, half, mine]

    def finish(row, carry):
        arrived = in_q.at[row, pl.ds(0, devices - 1)]
        pltpu.make_async_copy(arrived, arrived, br_sem.at[row]).wait()

        def predict_half(half, inner):
            predict(row, half)
            return inner

        def score_half(half, inner):
            score(row, half)
            return inner

        lax.fori_loop(0, halves, predict_half, 0)
        lax.fori_loop(0, halves, score_half, 0)
        return carry

    lax.fori_loop(0, rows, finish, 0)

    def deliver(index, carry):
        arrived = in_y.at[0, 0, pl.ds(0, members - 1)]
        pltpu.make_async_copy(arrived, arrived, zr_sem.at[index]).wait()
        pltpu.make_async_copy(arrived, arrived, ys_sem.at[index]).wait()
        pltpu.make_async_copy(arrived, arrived, zs_sem.at[index]).wait()
        return carry

    lax.fori_loop(0, rows * halves, deliver, 0)

    for part, (lane, width) in enumerate(chunks):
        sent = out_a.at[pl.ds(0, devices - 1), :, :, pl.ds(lane, width)]
        pltpu.make_async_copy(sent, sent, fs_sem.at[part]).wait()

    def drain(row, carry):
        sent = in_q.at[row, pl.ds(0, devices - 1)]
        pltpu.make_async_copy(sent, sent, bs_sem.at[row]).wait()
        return carry

    lax.fori_loop(0, rows, drain, 0)


def store(pred, slope, pred_out, slope_out, sem):
    copies = [
        pltpu.make_async_copy(pred, pred_out.at[0], sem.at[0]),
        pltpu.make_async_copy(slope, slope_out.at[0], sem.at[1]),
    ]
    for copy in copies:
        copy.start()
    for copy in copies:
        copy.wait()


def local(
    ensemble_starting_fields, observed, wave_of_slot, leg_forward, leg_inverse, spec_filter,
    gain_first, gain_second, weight_in, weight_out,
):
    _, rows, length, channels = ensemble_starting_fields.shape
    waves = wave_of_slot.shape[0]
    slots, degrees, lats = leg_forward.shape
    hidden = weight_in.shape[1]
    devices = lax.axis_size("lat")
    members = lax.axis_size("member")
    block = length // members
    parts = 2 * slots
    halves = 2
    forward, inverse = tables(waves, length)
    group = min(8, devices)
    order = group_order(group * rows, parts)
    whole = pl.BlockSpec(memory_space=pltpu.HBM)
    near = pl.BlockSpec(memory_space=pltpu.VMEM)
    sems = pltpu.SemaphoreType.DMA
    operands = [
        ensemble_starting_fields, observed, wave_of_slot, leg_forward, leg_inverse, spec_filter,
        gain_first, gain_second, weight_in, weight_out, forward, inverse, order,
    ]
    operands = [pltpu.with_memory_space_constraint(operand, pltpu.HBM) for operand in operands]
    pred, slope = pl.pallas_call(
        kernel,
        out_shape=(
            pltpu.VMEM((rows, length, channels), BF16),
            pltpu.VMEM((rows, members, block, channels), BF16),
        ),
        in_specs=[whole] * 13,
        out_specs=(near, near),
        scratch_shapes=[
            pltpu.VMEM((rows, length, channels), BF16),
            pltpu.VMEM((rows, block, channels), BF16),
            pltpu.VMEM((slots, degrees, lats), BF16),
            pltpu.VMEM((slots, lats, degrees), BF16),
            pltpu.VMEM((2, degrees, channels), F32),
            pltpu.VMEM((channels, hidden), BF16),
            pltpu.VMEM((hidden, channels), BF16),
            pltpu.VMEM((2 * waves, length), BF16),
            pltpu.VMEM((length, 2 * waves), BF16),
            pltpu.VMEM(order.shape, BF16),
            pltpu.VMEM((2 * waves, length), BF16),
            pltpu.VMEM((length, 2 * waves), BF16),
            pltpu.VMEM((rows, length, channels), BF16),
            pltpu.VMEM((devices, rows, parts, channels), BF16),
            pltpu.VMEM((devices, rows, parts, channels), BF16),
            pltpu.VMEM((parts, lats, channels), BF16),
            pltpu.VMEM((devices, rows, parts, channels), BF16),
            pltpu.VMEM((rows, devices, parts, channels), BF16),
            pltpu.VMEM((rows, halves, members, block // halves, channels), BF16),
            pltpu.VMEM((rows, halves, members, block // halves, channels), BF16),
            pltpu.VMEM((waves,), jnp.int32),
            pltpu.SMEM((waves,), jnp.int32),
            pltpu.VMEM((channels,), F32),
            pltpu.VMEM((channels,), F32),
            sems((9,)),
            sems((rows,)),
            sems((2,)),
            sems((2,)),
            sems((rows,)),
            sems((rows,)),
            sems((rows * halves,)),
            sems((rows * halves,)),
            sems((rows * halves,)),
            sems((rows * halves,)),
            sems((4,)),
        ],
        compiler_params=pltpu.CompilerParams(
            collective_id=0, has_side_effects=True, vmem_limit_bytes=48 * 1024 * 1024
        ),
    )(*operands)
    results = [pred, slope.reshape(rows, length, channels)]
    results = [pltpu.with_memory_space_constraint(result, pltpu.VMEM) for result in results]
    shape = jax.ShapeDtypeStruct((1, rows, length, channels), BF16)
    pred, slope = pl.pallas_call(
        store,
        out_shape=(shape, shape),
        in_specs=[near, near],
        out_specs=(whole, whole),
        scratch_shapes=[sems((2,))],
    )(*results)
    return (pred, slope)


def solution(mesh):
    in_specs = (
        P("member", "lat", None, None),
        P("lat", None, None),
        P(),
        P("lat", None, None),
        P("lat", None, None),
        P(),
        P(),
        P(),
        P(),
        P(),
    )
    out_specs = (P("member", "lat", None, None), P("member", "lat", None, None))
    return jax.shard_map(local, mesh=mesh, in_specs=in_specs, out_specs=out_specs, check_vma=False)
```

```python
import functools
import math

import jax
import jax.numpy as jnp
import numpy as np
from jax import lax
from jax.experimental import pallas as pl
from jax.experimental.pallas import tpu as pltpu
from jax.sharding import PartitionSpec as P

EPS_NORM = 1e-05
EPS_DIST = 1e-06
MESH = pl.DeviceIdType.MESH
F32 = jnp.float32
BF16 = jnp.bfloat16


def tables(waves, length):
    m = np.arange(waves)[:, None]
    j = np.arange(length)[None, :]
    angle = (m * j % length) * (2.0 * math.pi / length)
    cosine, sine = np.cos(angle), np.sin(angle)
    forward = np.stack([cosine / length, -sine / length], 1).reshape(2 * waves, length)
    weight = np.where(m == 0, 1.0, 2.0)
    inverse = np.stack([weight * cosine, -weight * sine], 1).reshape(2 * waves, length).T
    return jnp.asarray(forward, BF16), jnp.asarray(inverse, BF16)


def group_order(points, parts):
    rows = np.arange(points * parts)
    part, point = rows // points, rows % points
    order = np.zeros((points * parts, points * parts), np.float32)
    order[rows, point * parts + part] = 1.0
    return jnp.asarray(order, BF16)


def layer_norm(values, scales):
    average = jnp.mean(values, -1, keepdims=True)
    centred = values - average
    spread = jnp.mean(centred * centred, -1, keepdims=True)
    return centred * lax.rsqrt(spread + EPS_NORM) * scales


def inverse_distance(difference):
    return lax.rsqrt(jnp.mean(jnp.square(difference), -1, keepdims=True) + EPS_DIST)


def first_lanes(channels):
    return 2 * channels // 3 // 128 * 128


def dot(a, b):
    return jnp.dot(a, b, preferred_element_type=F32)


def kernel(
    x_hbm, obs_hbm, slot_hbm, legf_hbm, legi_hbm, filt_hbm, gain1_hbm, gain2_hbm, win_hbm, wout_hbm,
    cf_hbm, ci_hbm, order_hbm,
    pred, in_z,
    x, obs, legf, legi, filt, win, wout, cf, ci, order,
    fwd, inv, normed, out_a0, out_a1, in_r0, in_r1, spec, out_b, in_q, in_y, grad,
    slot_ref, slot_smem, gain1, gain2,
    load_sem, x_sem, fs_sem, fr_sem, bs_sem, br_sem, ys_sem, yr_sem, zs_sem, zr_sem, small_sem,
):
    members = lax.axis_size("member")
    devices = lax.axis_size("lat")
    me = lax.axis_index("lat")
    mine = lax.axis_index("member")
    rows, length, channels = x.shape
    degrees = legf.shape[1]
    parts = out_a0.shape[2]
    outs_a, ins_r = [out_a0, out_a1], [in_r0, in_r1]
    slots = parts // 2
    block = length // members
    stride = 1

    def lat_peer(step):
        return (me + stride * step) % devices

    x_loads = [
        pltpu.make_async_copy(x_hbm.at[0, row], x.at[row], x_sem.at[row]) for row in range(rows)
    ]
    sources = [cf_hbm, ci_hbm, order_hbm, legf_hbm, legi_hbm, filt_hbm, win_hbm, wout_hbm]
    places = [cf, ci, order, legf, legi, filt, win, wout]
    loads = [
        pltpu.make_async_copy(source, place, load_sem.at[index])
        for index, (source, place) in enumerate(zip(sources, places))
    ]
    obs_load = pltpu.make_async_copy(
        obs_hbm.at[:, pl.ds(pl.multiple_of(mine * block, block), block), :],
        obs,
        load_sem.at[len(loads)],
    )
    small = [
        pltpu.make_async_copy(source, place, small_sem.at[index])
        for index, (source, place) in enumerate(
            [(slot_hbm, slot_ref), (gain1_hbm, gain1), (gain2_hbm, gain2), (slot_hbm, slot_smem)]
        )
    ]
    for load in small:
        load.start()
    loads[0].start()
    for load in x_loads:
        load.start()
    for load in loads[1:]:
        load.start()
    obs_load.start()

    barrier = pltpu.get_barrier_semaphore()

    def greet(step, carry):
        pl.semaphore_signal(barrier, inc=1, device_id=(mine, lat_peer(step)), device_id_type=MESH)
        return carry

    lax.fori_loop(devices // 2, devices, greet, 0)
    lax.fori_loop(1, devices // 2, greet, 0)
    for step in range(1, members):
        pl.semaphore_signal(
            barrier, inc=1, device_id=((mine + step) % members, me), device_id_type=MESH
        )

    for load in small:
        load.wait()
    spread = (degrees, 2 * degrees)
    gap = lax.broadcasted_iota(jnp.int32, spread, 1) - 2 * lax.broadcasted_iota(jnp.int32, spread, 0)
    twice = jnp.where((gap == 0) | (gap == 1), 2.0, 0.0).astype(BF16)
    waves = jnp.broadcast_to(slot_ref[...].astype(F32)[None, :], (8, degrees)).astype(BF16)
    columns = dot(waves, twice)[0:1].astype(jnp.int32)
    square = (2 * degrees, 2 * degrees)
    columns = columns + lax.broadcasted_iota(jnp.int32, (1, 2 * degrees), 1) % 2
    picked = jnp.where(lax.broadcasted_iota(jnp.int32, square, 0) == columns, 1.0, 0.0).astype(BF16)
    loads[0].wait()
    fwd[...] = lax.dot_general(
        picked, cf[...], (((0,), (0,)), ((), ())), preferred_element_type=F32
    ).astype(BF16)

    first = first_lanes(channels)
    chunks = [(0, first), (first, channels - first)]

    def norm_rows(row, carry):
        def norm_tile(tile, inner):
            at = pl.ds(pl.multiple_of(tile * wide, wide), wide)
            normed[row, at, :] = layer_norm(x[row, at, :].astype(F32), gain1[...][None, :]).astype(BF16)
            return inner

        return lax.fori_loop(0, length // wide, norm_tile, carry)

    wide = min(256, length)

    for row in range(rows):
        x_loads[row].wait()
        norm_rows(row, 0)

    for part, (lane, width) in enumerate(chunks):
        lanes = pl.ds(lane, width)
        out_a, in_r = outs_a[part], ins_r[part]

        def analyse(row, carry):
            found = dot(fwd[...], normed[row, :, lanes]).astype(BF16)
            out_a[:, row] = found.reshape(devices, parts, width)
            return carry

        lax.fori_loop(0, rows, analyse, 0)
        if part == 0:
            pl.semaphore_wait(barrier, devices - 1 + members - 1)

        def send(step, carry):
            peer = lat_peer(step)
            pltpu.make_async_remote_copy(
                src_ref=out_a.at[peer],
                dst_ref=in_r.at[me],
                send_sem=fs_sem.at[part],
                recv_sem=fr_sem.at[part],
                device_id=(mine, peer),
                device_id_type=MESH,
            ).start()
            return carry

        lax.fori_loop(1, devices, send, 0)
        in_r[me] = out_a[me]

    loads[1].wait()
    inv[...] = dot(ci[...], picked).astype(BF16)
    for load in loads[2:]:
        load.wait()
    for slot in range(slots):
        local = slot_smem[me * slots + slot]
        level = lax.broadcasted_iota(jnp.int32, (degrees, degrees), 0)
        kept = legf[slot].astype(F32)
        legf[slot] = jnp.where(level >= local, kept, 0.0).astype(BF16)

    group = order.shape[0] // (rows * parts)
    points = group * rows

    def send_back(row, lanes):
        def send(step, carry):
            peer = lat_peer(step)
            pltpu.make_async_remote_copy(
                src_ref=out_b.at[peer, row, :, lanes],
                dst_ref=in_q.at[row, me, :, lanes],
                send_sem=bs_sem.at[row],
                recv_sem=br_sem.at[row],
                device_id=(mine, peer),
                device_id_type=MESH,
            ).start()
            return carry

        lax.fori_loop(1, devices, send, 0)

    for part, (lane, width) in enumerate(chunks):
        lanes = pl.ds(lane, width)
        in_r = ins_r[part]
        everything = in_r.at[pl.ds(0, devices - 1)]
        pltpu.make_async_copy(everything, everything, fr_sem.at[part]).wait()

        def gather(index, carry):
            taken = in_r[pl.ds(index * group, group)].reshape(points * parts, width)
            moved = dot(order[...], taken).astype(BF16)
            at = pl.ds(pl.multiple_of(index * points, points), points)
            spec[:, at, lanes] = moved.reshape(parts, points, width)
            return carry

        lax.fori_loop(0, devices // group, gather, 0)

        def transform(slot, carry):
            real = dot(legf[slot], spec[2 * slot, :, lanes])
            imag = dot(legf[slot], spec[2 * slot + 1, :, lanes])
            filt_real, filt_imag = filt[0, :, lanes], filt[1, :, lanes]
            new_real = (real * filt_real - imag * filt_imag).astype(BF16)
            new_imag = (real * filt_imag + imag * filt_real).astype(BF16)
            spec[2 * slot, :, lanes] = dot(legi[slot], new_real).astype(BF16)
            spec[2 * slot + 1, :, lanes] = dot(legi[slot], new_imag).astype(BF16)
            return carry

        lax.fori_loop(0, slots, transform, 0)

        def scatter(index, carry):
            at = pl.ds(pl.multiple_of(index * points, points), points)
            taken = spec[:, at, lanes].reshape(points * parts, width)
            moved = lax.dot_general(
                order[...], taken, (((0,), (0,)), ((), ())), preferred_element_type=F32
            ).astype(BF16)
            out_b[pl.ds(index * group, group), :, :, lanes] = moved.reshape(group, rows, parts, width)
            return carry

        lax.fori_loop(0, devices // group, scatter, 0)
        send_back(0, lanes)

    everywhere = pl.ds(0, channels)

    def send_rest(row, carry):
        send_back(row, everywhere)
        return carry

    lax.fori_loop(1, rows, send_rest, 0)
    for row in range(rows):
        in_q[row, me] = out_b[me, row]
    obs_load.wait()

    halves = in_y.shape[1]
    piece = block // halves
    thin = min(32, piece)

    def spans(half):
        return [
            pl.ds(pl.multiple_of(index * block + half * piece, piece), piece)
            for index in range(members)
        ]

    def predict(row, half):
        waves = in_q[row].reshape(devices * parts, channels)
        table = jnp.concatenate([inv[at, :] for at in spans(half)], 0)
        before = jnp.concatenate([x[row, at, :] for at in spans(half)], 0)
        after = before.astype(F32) + dot(table, waves)
        second = layer_norm(after, gain2[...][None, :]).astype(BF16)
        hidden = jax.nn.gelu(dot(second, win[...])).astype(BF16)
        result = (after + dot(hidden, wout[...])).astype(BF16)
        for index, at in enumerate(spans(half)):
            pred[row, at, :] = result[index * piece : (index + 1) * piece]
        for step in range(1, members):
            peer = (mine + step) % members
            pltpu.make_async_remote_copy(
                src_ref=pred.at[row, pl.ds(pl.multiple_of(peer * block + half * piece, piece), piece), :],
                dst_ref=in_y.at[row, half, mine],
                send_sem=ys_sem.at[row * halves + half],
                recv_sem=yr_sem.at[row * halves + half],
                device_id=(peer, me),
                device_id_type=MESH,
            ).start()

    def score(row, half):
        arrived = in_y.at[row, half, pl.ds(0, members - 1)]
        pltpu.make_async_copy(arrived, arrived, yr_sem.at[row * halves + half]).wait()
        own = pl.ds(pl.multiple_of(mine * block + half * piece, piece), piece)
        in_y[row, half, mine] = pred[row, own, :]

        def score_rows(tile, carry):
            at = pl.ds(pl.multiple_of(tile * thin, thin), thin)
            fields = [in_y[row, half, index, at, :].astype(F32) for index in range(members)]
            here = pl.ds(pl.multiple_of(half * piece + tile * thin, thin), thin)
            target = obs[row, here, :].astype(F32)
            slopes = []
            for index in range(members):
                gap = fields[index] - target
                slopes.append(gap * inverse_distance(gap))
            for one in range(members):
                for two in range(one + 1, members):
                    gap = fields[one] - fields[two]
                    pull = gap * (inverse_distance(gap) * (1.0 / (members - 1)))
                    slopes[one] = slopes[one] - pull
                    slopes[two] = slopes[two] + pull
            for index in range(members):
                grad[row, half, index, at, :] = slopes[index].astype(BF16)
            return carry

        lax.fori_loop(0, piece // thin, score_rows, 0)
        there = pl.ds(pl.multiple_of(half * piece, piece), piece)
        for step in range(1, members):
            peer = (mine + step) % members
            pltpu.make_async_remote_copy(
                src_ref=grad.at[row, half, peer],
                dst_ref=in_z.at[row, mine, there, :],
                send_sem=zs_sem.at[row * halves + half],
                recv_sem=zr_sem.at[row * halves + half],
                device_id=(peer, me),
                device_id_type=MESH,
            ).start()
        in_z[row, mine, there, :] = grad[row, half, mine]

    def finish(row, carry):
        arrived = in_q.at[row, pl.ds(0, devices - 1)]
        pltpu.make_async_copy(arrived, arrived, br_sem.at[row]).wait()

        def predict_half(half, inner):
            predict(row, half)
            return inner

        def score_half(half, inner):
            score(row, half)
            return inner

        lax.fori_loop(0, halves, predict_half, 0)
        lax.fori_loop(0, halves, score_half, 0)
        return carry

    lax.fori_loop(0, rows, finish, 0)

    def deliver(index, carry):
        arrived = in_y.at[0, 0, pl.ds(0, members - 1)]
        pltpu.make_async_copy(arrived, arrived, zr_sem.at[index]).wait()
        pltpu.make_async_copy(arrived, arrived, ys_sem.at[index]).wait()
        pltpu.make_async_copy(arrived, arrived, zs_sem.at[index]).wait()
        return carry

    lax.fori_loop(0, rows * halves, deliver, 0)

    for part, (lane, width) in enumerate(chunks):
        sent = outs_a[part].at[pl.ds(0, devices - 1)]
        pltpu.make_async_copy(sent, sent, fs_sem.at[part]).wait()

    def drain(row, carry):
        sent = in_q.at[row, pl.ds(0, devices - 1)]
        pltpu.make_async_copy(sent, sent, bs_sem.at[row]).wait()
        return carry

    lax.fori_loop(0, rows, drain, 0)


def store(pred, slope, pred_out, slope_out, sem):
    copies = [
        pltpu.make_async_copy(pred, pred_out.at[0], sem.at[0]),
        pltpu.make_async_copy(slope, slope_out.at[0], sem.at[1]),
    ]
    for copy in copies:
        copy.start()
    for copy in copies:
        copy.wait()


def local(
    ensemble_starting_fields, observed, wave_of_slot, leg_forward, leg_inverse, spec_filter,
    gain_first, gain_second, weight_in, weight_out,
):
    _, rows, length, channels = ensemble_starting_fields.shape
    waves = wave_of_slot.shape[0]
    slots, degrees, lats = leg_forward.shape
    hidden = weight_in.shape[1]
    devices = lax.axis_size("lat")
    members = lax.axis_size("member")
    block = length // members
    parts = 2 * slots
    halves = 2
    first = first_lanes(channels)
    forward, inverse = tables(waves, length)
    group = min(8, devices)
    order = group_order(group * rows, parts)
    whole = pl.BlockSpec(memory_space=pltpu.HBM)
    near = pl.BlockSpec(memory_space=pltpu.VMEM)
    sems = pltpu.SemaphoreType.DMA
    operands = [
        ensemble_starting_fields, observed, wave_of_slot, leg_forward, leg_inverse, spec_filter,
        gain_first, gain_second, weight_in, weight_out, forward, inverse, order,
    ]
    operands = [pltpu.with_memory_space_constraint(operand, pltpu.HBM) for operand in operands]
    pred, slope = pl.pallas_call(
        kernel,
        out_shape=(
            pltpu.VMEM((rows, length, channels), BF16),
            pltpu.VMEM((rows, members, block, channels), BF16),
        ),
        in_specs=[whole] * 13,
        out_specs=(near, near),
        scratch_shapes=[
            pltpu.VMEM((rows, length, channels), BF16),
            pltpu.VMEM((rows, block, channels), BF16),
            pltpu.VMEM((slots, degrees, lats), BF16),
            pltpu.VMEM((slots, lats, degrees), BF16),
            pltpu.VMEM((2, degrees, channels), F32),
            pltpu.VMEM((channels, hidden), BF16),
            pltpu.VMEM((hidden, channels), BF16),
            pltpu.VMEM((2 * waves, length), BF16),
            pltpu.VMEM((length, 2 * waves), BF16),
            pltpu.VMEM(order.shape, BF16),
            pltpu.VMEM((2 * waves, length), BF16),
            pltpu.VMEM((length, 2 * waves), BF16),
            pltpu.VMEM((rows, length, channels), BF16),
            pltpu.VMEM((devices, rows, parts, first), BF16),
            pltpu.VMEM((devices, rows, parts, channels - first), BF16),
            pltpu.VMEM((devices, rows, parts, first), BF16),
            pltpu.VMEM((devices, rows, parts, channels - first), BF16),
            pltpu.VMEM((parts, lats, channels), BF16),
            pltpu.VMEM((devices, rows, parts, channels), BF16),
            pltpu.VMEM((rows, devices, parts, channels), BF16),
            pltpu.VMEM((rows, halves, members, block // halves, channels), BF16),
            pltpu.VMEM((rows, halves, members, block // halves, channels), BF16),
            pltpu.VMEM((waves,), jnp.int32),
            pltpu.SMEM((waves,), jnp.int32),
            pltpu.VMEM((channels,), F32),
            pltpu.VMEM((channels,), F32),
            sems((9,)),
            sems((rows,)),
            sems((2,)),
            sems((2,)),
            sems((rows,)),
            sems((rows,)),
            sems((rows * halves,)),
            sems((rows * halves,)),
            sems((rows * halves,)),
            sems((rows * halves,)),
            sems((4,)),
        ],
        compiler_params=pltpu.CompilerParams(
            collective_id=0, has_side_effects=True, vmem_limit_bytes=48 * 1024 * 1024
        ),
    )(*operands)
    results = [pred, slope.reshape(rows, length, channels)]
    results = [pltpu.with_memory_space_constraint(result, pltpu.VMEM) for result in results]
    shape = jax.ShapeDtypeStruct((1, rows, length, channels), BF16)
    pred, slope = pl.pallas_call(
        store,
        out_shape=(shape, shape),
        in_specs=[near, near],
        out_specs=(whole, whole),
        scratch_shapes=[sems((2,))],
    )(*results)
    return (pred, slope)


def solution(mesh):
    in_specs = (
        P("member", "lat", None, None),
        P("lat", None, None),
        P(),
        P("lat", None, None),
        P("lat", None, None),
        P(),
        P(),
        P(),
        P(),
        P(),
    )
    out_specs = (P("member", "lat", None, None), P("member", "lat", None, None))
    return jax.shard_map(local, mesh=mesh, in_specs=in_specs, out_specs=out_specs, check_vma=False)
```

```python
import functools
import math

import jax
import jax.numpy as jnp
import numpy as np
from jax import lax
from jax.experimental import pallas as pl
from jax.experimental.pallas import tpu as pltpu
from jax.sharding import PartitionSpec as P

EPS_NORM = 1e-05
EPS_DIST = 1e-06
MESH = pl.DeviceIdType.MESH
F32 = jnp.float32
BF16 = jnp.bfloat16


def tables(waves, length):
    m = np.arange(waves)[:, None]
    j = np.arange(length)[None, :]
    angle = (m * j % length) * (2.0 * math.pi / length)
    cosine, sine = np.cos(angle), np.sin(angle)
    forward = np.stack([cosine / length, -sine / length], 1).reshape(2 * waves, length)
    weight = np.where(m == 0, 1.0, 2.0)
    inverse = np.stack([weight * cosine, -weight * sine], 1).reshape(2 * waves, length).T
    return jnp.asarray(forward, BF16), jnp.asarray(inverse, BF16)


def group_order(points, parts):
    rows = np.arange(points * parts)
    part, point = rows // points, rows % points
    order = np.zeros((points * parts, points * parts), np.float32)
    order[rows, point * parts + part] = 1.0
    return jnp.asarray(order, BF16)


def layer_norm(values, scales):
    average = jnp.mean(values, -1, keepdims=True)
    centred = values - average
    spread = jnp.mean(centred * centred, -1, keepdims=True)
    return centred * lax.rsqrt(spread + EPS_NORM) * scales


def inverse_distance(difference):
    return lax.rsqrt(jnp.mean(jnp.square(difference), -1, keepdims=True) + EPS_DIST)


def first_lanes(channels):
    return 2 * channels // 3 // 128 * 128


def dot(a, b):
    return jnp.dot(a, b, preferred_element_type=F32)


def kernel(
    x_hbm, obs_hbm, slot_hbm, legf_hbm, legi_hbm, filt_hbm, gain1_hbm, gain2_hbm, win_hbm, wout_hbm,
    cf_hbm, ci_hbm, order_hbm,
    pred, in_z,
    x, obs, legf, legi, filt, win, wout, cf, ci, order,
    fwd, inv, normed, out_a0, out_a1, in_r0, in_r1, spec, out_b, in_q, in_y, grad,
    slot_ref, slot_smem, gain1, gain2,
    load_sem, x_sem, fs_sem, fr_sem, bs_sem, br_sem, ys_sem, yr_sem, zs_sem, zr_sem, small_sem,
):
    members = lax.axis_size("member")
    devices = lax.axis_size("lat")
    me = lax.axis_index("lat")
    mine = lax.axis_index("member")
    rows, length, channels = x.shape
    degrees = legf.shape[1]
    parts = out_a0.shape[2]
    outs_a, ins_r = [out_a0, out_a1], [in_r0, in_r1]
    slots = parts // 2
    block = length // members
    stride = 1

    def lat_peer(step):
        return (me + stride * step) % devices

    x_loads = [
        pltpu.make_async_copy(x_hbm.at[0, row], x.at[row], x_sem.at[row]) for row in range(rows)
    ]
    sources = [cf_hbm, ci_hbm, order_hbm, legf_hbm, legi_hbm, filt_hbm, win_hbm, wout_hbm]
    places = [cf, ci, order, legf, legi, filt, win, wout]
    loads = [
        pltpu.make_async_copy(source, place, load_sem.at[index])
        for index, (source, place) in enumerate(zip(sources, places))
    ]
    obs_load = pltpu.make_async_copy(
        obs_hbm.at[:, pl.ds(pl.multiple_of(mine * block, block), block), :],
        obs,
        load_sem.at[len(loads)],
    )
    small = [
        pltpu.make_async_copy(source, place, small_sem.at[index])
        for index, (source, place) in enumerate(
            [(slot_hbm, slot_ref), (gain1_hbm, gain1), (gain2_hbm, gain2), (slot_hbm, slot_smem)]
        )
    ]
    for load in small:
        load.start()
    loads[0].start()
    for load in x_loads:
        load.start()
    for load in loads[1:]:
        load.start()
    obs_load.start()

    barrier = pltpu.get_barrier_semaphore()

    def greet(step, carry):
        pl.semaphore_signal(barrier, inc=1, device_id=(mine, lat_peer(step)), device_id_type=MESH)
        return carry

    lax.fori_loop(devices // 2, devices, greet, 0)
    lax.fori_loop(1, devices // 2, greet, 0)
    for step in range(1, members):
        pl.semaphore_signal(
            barrier, inc=1, device_id=((mine + step) % members, me), device_id_type=MESH
        )

    for load in small:
        load.wait()
    spread = (degrees, 2 * degrees)
    gap = lax.broadcasted_iota(jnp.int32, spread, 1) - 2 * lax.broadcasted_iota(jnp.int32, spread, 0)
    twice = jnp.where((gap == 0) | (gap == 1), 2.0, 0.0).astype(BF16)
    waves = jnp.broadcast_to(slot_ref[...].astype(F32)[None, :], (8, degrees)).astype(BF16)
    columns = dot(waves, twice)[0:1].astype(jnp.int32)
    square = (2 * degrees, 2 * degrees)
    columns = columns + lax.broadcasted_iota(jnp.int32, (1, 2 * degrees), 1) % 2
    picked = jnp.where(lax.broadcasted_iota(jnp.int32, square, 0) == columns, 1.0, 0.0).astype(BF16)
    loads[0].wait()
    fwd[...] = lax.dot_general(
        picked, cf[...], (((0,), (0,)), ((), ())), preferred_element_type=F32
    ).astype(BF16)

    first = first_lanes(channels)
    chunks = [(0, first), (first, channels - first)]

    def norm_rows(row, carry):
        def norm_tile(tile, inner):
            at = pl.ds(pl.multiple_of(tile * wide, wide), wide)
            normed[row, at, :] = layer_norm(x[row, at, :].astype(F32), gain1[...][None, :]).astype(BF16)
            return inner

        return lax.fori_loop(0, length // wide, norm_tile, carry)

    wide = min(256, length)

    for row in range(rows):
        x_loads[row].wait()
        norm_rows(row, 0)

    for part, (lane, width) in enumerate(chunks):
        lanes = pl.ds(lane, width)
        out_a, in_r = outs_a[part], ins_r[part]

        def analyse(row, carry):
            found = dot(fwd[...], normed[row, :, lanes]).astype(BF16)
            out_a[:, row] = found.reshape(devices, parts, width)
            return carry

        lax.fori_loop(0, rows, analyse, 0)
        if part == 0:
            pl.semaphore_wait(barrier, devices - 1 + members - 1)

        def send(step, carry):
            peer = lat_peer(step)
            pltpu.make_async_remote_copy(
                src_ref=out_a.at[peer],
                dst_ref=in_r.at[me],
                send_sem=fs_sem.at[part],
                recv_sem=fr_sem.at[part],
                device_id=(mine, peer),
                device_id_type=MESH,
            ).start()
            return carry

        lax.fori_loop(1, devices, send, 0)
        in_r[me] = out_a[me]

    loads[1].wait()
    inv[...] = dot(ci[...], picked).astype(BF16)
    for load in loads[2:]:
        load.wait()
    for slot in range(slots):
        local = slot_smem[me * slots + slot]
        level = lax.broadcasted_iota(jnp.int32, (degrees, degrees), 0)
        kept = legf[slot].astype(F32)
        legf[slot] = jnp.where(level >= local, kept, 0.0).astype(BF16)

    group = order.shape[0] // (rows * parts)
    points = group * rows

    def send_back(row, lanes):
        def send(step, carry):
            peer = lat_peer(step)
            pltpu.make_async_remote_copy(
                src_ref=out_b.at[peer, row, :, lanes],
                dst_ref=in_q.at[row, me, :, lanes],
                send_sem=bs_sem.at[row],
                recv_sem=br_sem.at[row],
                device_id=(mine, peer),
                device_id_type=MESH,
            ).start()
            return carry

        lax.fori_loop(1, devices, send, 0)

    for part, (lane, width) in enumerate(chunks):
        lanes = pl.ds(lane, width)
        in_r = ins_r[part]
        everything = in_r.at[pl.ds(0, devices - 1)]
        pltpu.make_async_copy(everything, everything, fr_sem.at[part]).wait()

        def gather(index, carry):
            taken = in_r[pl.ds(index * group, group)].reshape(points * parts, width)
            moved = dot(order[...], taken).astype(BF16)
            at = pl.ds(pl.multiple_of(index * points, points), points)
            spec[:, at, lanes] = moved.reshape(parts, points, width)
            return carry

        lax.fori_loop(0, devices // group, gather, 0)

        def transform(slot, carry):
            real = dot(legf[slot], spec[2 * slot, :, lanes])
            imag = dot(legf[slot], spec[2 * slot + 1, :, lanes])
            filt_real, filt_imag = filt[0, :, lanes], filt[1, :, lanes]
            new_real = (real * filt_real - imag * filt_imag).astype(BF16)
            new_imag = (real * filt_imag + imag * filt_real).astype(BF16)
            spec[2 * slot, :, lanes] = dot(legi[slot], new_real).astype(BF16)
            spec[2 * slot + 1, :, lanes] = dot(legi[slot], new_imag).astype(BF16)
            return carry

        lax.fori_loop(0, slots, transform, 0)

        def scatter(index, carry):
            at = pl.ds(pl.multiple_of(index * points, points), points)
            taken = spec[:, at, lanes].reshape(points * parts, width)
            moved = lax.dot_general(
                order[...], taken, (((0,), (0,)), ((), ())), preferred_element_type=F32
            ).astype(BF16)
            out_b[pl.ds(index * group, group), :, :, lanes] = moved.reshape(group, rows, parts, width)
            return carry

        lax.fori_loop(0, devices // group, scatter, 0)
        send_back(0, lanes)

    everywhere = pl.ds(0, channels)

    ahead = min(2, rows)
    for row in range(1, ahead):
        send_back(row, everywhere)
    for row in range(rows):
        in_q[row, me] = out_b[me, row]
    obs_load.wait()

    halves = in_y.shape[1]
    piece = block // halves
    thin = min(32, piece)

    def spans(half):
        return [
            pl.ds(pl.multiple_of(index * block + half * piece, piece), piece)
            for index in range(members)
        ]

    def predict(row, half):
        waves = in_q[row].reshape(devices * parts, channels)
        table = jnp.concatenate([inv[at, :] for at in spans(half)], 0)
        before = jnp.concatenate([x[row, at, :] for at in spans(half)], 0)
        after = before.astype(F32) + dot(table, waves)
        second = layer_norm(after, gain2[...][None, :]).astype(BF16)
        hidden = jax.nn.gelu(dot(second, win[...])).astype(BF16)
        result = (after + dot(hidden, wout[...])).astype(BF16)
        for index, at in enumerate(spans(half)):
            pred[row, at, :] = result[index * piece : (index + 1) * piece]
        for step in range(1, members):
            peer = (mine + step) % members
            pltpu.make_async_remote_copy(
                src_ref=pred.at[row, pl.ds(pl.multiple_of(peer * block + half * piece, piece), piece), :],
                dst_ref=in_y.at[row, half, mine],
                send_sem=ys_sem.at[row * halves + half],
                recv_sem=yr_sem.at[row * halves + half],
                device_id=(peer, me),
                device_id_type=MESH,
            ).start()

    def score(row, half):
        arrived = in_y.at[row, half, pl.ds(0, members - 1)]
        pltpu.make_async_copy(arrived, arrived, yr_sem.at[row * halves + half]).wait()
        own = pl.ds(pl.multiple_of(mine * block + half * piece, piece), piece)
        in_y[row, half, mine] = pred[row, own, :]

        def score_rows(tile, carry):
            at = pl.ds(pl.multiple_of(tile * thin, thin), thin)
            fields = [in_y[row, half, index, at, :].astype(F32) for index in range(members)]
            here = pl.ds(pl.multiple_of(half * piece + tile * thin, thin), thin)
            target = obs[row, here, :].astype(F32)
            slopes = []
            for index in range(members):
                gap = fields[index] - target
                slopes.append(gap * inverse_distance(gap))
            for one in range(members):
                for two in range(one + 1, members):
                    gap = fields[one] - fields[two]
                    pull = gap * (inverse_distance(gap) * (1.0 / (members - 1)))
                    slopes[one] = slopes[one] - pull
                    slopes[two] = slopes[two] + pull
            for index in range(members):
                grad[row, half, index, at, :] = slopes[index].astype(BF16)
            return carry

        lax.fori_loop(0, piece // thin, score_rows, 0)
        there = pl.ds(pl.multiple_of(half * piece, piece), piece)
        for step in range(1, members):
            peer = (mine + step) % members
            pltpu.make_async_remote_copy(
                src_ref=grad.at[row, half, peer],
                dst_ref=in_z.at[row, mine, there, :],
                send_sem=zs_sem.at[row * halves + half],
                recv_sem=zr_sem.at[row * halves + half],
                device_id=(peer, me),
                device_id_type=MESH,
            ).start()
        in_z[row, mine, there, :] = grad[row, half, mine]

    def wait_sent(row):
        sent = in_q.at[row, pl.ds(0, devices - 1)]
        pltpu.make_async_copy(sent, sent, bs_sem.at[row]).wait()

    def finish(row, carry):
        arrived = in_q.at[row, pl.ds(0, devices - 1)]
        pltpu.make_async_copy(arrived, arrived, br_sem.at[row]).wait()

        def predict_half(half, inner):
            predict(row, half)
            return inner

        def score_half(half, inner):
            score(row, half)
            return inner

        lax.fori_loop(0, halves, predict_half, 0)

        @pl.when(row + ahead < rows)
        def _():
            wait_sent(row)
            send_back(row + ahead, everywhere)

        lax.fori_loop(0, halves, score_half, 0)
        return carry

    lax.fori_loop(0, rows, finish, 0)

    def deliver(index, carry):
        arrived = in_y.at[0, 0, pl.ds(0, members - 1)]
        pltpu.make_async_copy(arrived, arrived, zr_sem.at[index]).wait()
        pltpu.make_async_copy(arrived, arrived, ys_sem.at[index]).wait()
        pltpu.make_async_copy(arrived, arrived, zs_sem.at[index]).wait()
        return carry

    lax.fori_loop(0, rows * halves, deliver, 0)

    for part, (lane, width) in enumerate(chunks):
        sent = outs_a[part].at[pl.ds(0, devices - 1)]
        pltpu.make_async_copy(sent, sent, fs_sem.at[part]).wait()

    def drain(row, carry):
        wait_sent(row)
        return carry

    lax.fori_loop(rows - ahead, rows, drain, 0)


def store(pred, slope, pred_out, slope_out, sem):
    copies = [
        pltpu.make_async_copy(pred, pred_out.at[0], sem.at[0]),
        pltpu.make_async_copy(slope, slope_out.at[0], sem.at[1]),
    ]
    for copy in copies:
        copy.start()
    for copy in copies:
        copy.wait()


def local(
    ensemble_starting_fields, observed, wave_of_slot, leg_forward, leg_inverse, spec_filter,
    gain_first, gain_second, weight_in, weight_out,
):
    _, rows, length, channels = ensemble_starting_fields.shape
    waves = wave_of_slot.shape[0]
    slots, degrees, lats = leg_forward.shape
    hidden = weight_in.shape[1]
    devices = lax.axis_size("lat")
    members = lax.axis_size("member")
    block = length // members
    parts = 2 * slots
    halves = 2
    first = first_lanes(channels)
    forward, inverse = tables(waves, length)
    group = min(8, devices)
    order = group_order(group * rows, parts)
    whole = pl.BlockSpec(memory_space=pltpu.HBM)
    near = pl.BlockSpec(memory_space=pltpu.VMEM)
    sems = pltpu.SemaphoreType.DMA
    operands = [
        ensemble_starting_fields, observed, wave_of_slot, leg_forward, leg_inverse, spec_filter,
        gain_first, gain_second, weight_in, weight_out, forward, inverse, order,
    ]
    operands = [pltpu.with_memory_space_constraint(operand, pltpu.HBM) for operand in operands]
    pred, slope = pl.pallas_call(
        kernel,
        out_shape=(
            pltpu.VMEM((rows, length, channels), BF16),
            pltpu.VMEM((rows, members, block, channels), BF16),
        ),
        in_specs=[whole] * 13,
        out_specs=(near, near),
        scratch_shapes=[
            pltpu.VMEM((rows, length, channels), BF16),
            pltpu.VMEM((rows, block, channels), BF16),
            pltpu.VMEM((slots, degrees, lats), BF16),
            pltpu.VMEM((slots, lats, degrees), BF16),
            pltpu.VMEM((2, degrees, channels), F32),
            pltpu.VMEM((channels, hidden), BF16),
            pltpu.VMEM((hidden, channels), BF16),
            pltpu.VMEM((2 * waves, length), BF16),
            pltpu.VMEM((length, 2 * waves), BF16),
            pltpu.VMEM(order.shape, BF16),
            pltpu.VMEM((2 * waves, length), BF16),
            pltpu.VMEM((length, 2 * waves), BF16),
            pltpu.VMEM((rows, length, channels), BF16),
            pltpu.VMEM((devices, rows, parts, first), BF16),
            pltpu.VMEM((devices, rows, parts, channels - first), BF16),
            pltpu.VMEM((devices, rows, parts, first), BF16),
            pltpu.VMEM((devices, rows, parts, channels - first), BF16),
            pltpu.VMEM((parts, lats, channels), BF16),
            pltpu.VMEM((devices, rows, parts, channels), BF16),
            pltpu.VMEM((rows, devices, parts, channels), BF16),
            pltpu.VMEM((rows, halves, members, block // halves, channels), BF16),
            pltpu.VMEM((rows, halves, members, block // halves, channels), BF16),
            pltpu.VMEM((waves,), jnp.int32),
            pltpu.SMEM((waves,), jnp.int32),
            pltpu.VMEM((channels,), F32),
            pltpu.VMEM((channels,), F32),
            sems((9,)),
            sems((rows,)),
            sems((2,)),
            sems((2,)),
            sems((rows,)),
            sems((rows,)),
            sems((rows * halves,)),
            sems((rows * halves,)),
            sems((rows * halves,)),
            sems((rows * halves,)),
            sems((4,)),
        ],
        compiler_params=pltpu.CompilerParams(
            collective_id=0, has_side_effects=True, vmem_limit_bytes=48 * 1024 * 1024
        ),
    )(*operands)
    results = [pred, slope.reshape(rows, length, channels)]
    results = [pltpu.with_memory_space_constraint(result, pltpu.VMEM) for result in results]
    shape = jax.ShapeDtypeStruct((1, rows, length, channels), BF16)
    pred, slope = pl.pallas_call(
        store,
        out_shape=(shape, shape),
        in_specs=[near, near],
        out_specs=(whole, whole),
        scratch_shapes=[sems((2,))],
    )(*results)
    return (pred, slope)


def solution(mesh):
    in_specs = (
        P("member", "lat", None, None),
        P("lat", None, None),
        P(),
        P("lat", None, None),
        P("lat", None, None),
        P(),
        P(),
        P(),
        P(),
        P(),
    )
    out_specs = (P("member", "lat", None, None), P("member", "lat", None, None))
    return jax.shard_map(local, mesh=mesh, in_specs=in_specs, out_specs=out_specs, check_vma=False)
```

```python
import functools
import math

import jax
import jax.numpy as jnp
import numpy as np
from jax import lax
from jax.experimental import pallas as pl
from jax.experimental.pallas import tpu as pltpu
from jax.sharding import PartitionSpec as P

EPS_NORM = 1e-05
EPS_DIST = 1e-06
MESH = pl.DeviceIdType.MESH
F32 = jnp.float32
BF16 = jnp.bfloat16


def tables(waves, length):
    m = np.arange(waves)[:, None]
    j = np.arange(length)[None, :]
    angle = (m * j % length) * (2.0 * math.pi / length)
    cosine, sine = np.cos(angle), np.sin(angle)
    forward = np.stack([cosine / length, -sine / length], 1).reshape(2 * waves, length)
    weight = np.where(m == 0, 1.0, 2.0)
    inverse = np.stack([weight * cosine, -weight * sine], 1).reshape(2 * waves, length).T
    return jnp.asarray(forward, BF16), jnp.asarray(inverse, BF16)


def group_order(points, parts):
    rows = np.arange(points * parts)
    part, point = rows // points, rows % points
    order = np.zeros((points * parts, points * parts), np.float32)
    order[rows, point * parts + part] = 1.0
    return jnp.asarray(order, BF16)


def layer_norm(values, scales):
    average = jnp.mean(values, -1, keepdims=True)
    centred = values - average
    spread = jnp.mean(centred * centred, -1, keepdims=True)
    return centred * lax.rsqrt(spread + EPS_NORM) * scales


def inverse_distance(difference):
    return lax.rsqrt(jnp.mean(jnp.square(difference), -1, keepdims=True) + EPS_DIST)


def first_lanes(channels):
    return 2 * channels // 3 // 128 * 128


def dot(a, b):
    return jnp.dot(a, b, preferred_element_type=F32)


def kernel(
    x_hbm, obs_hbm, slot_hbm, legf_hbm, legi_hbm, filt_hbm, gain1_hbm, gain2_hbm, win_hbm, wout_hbm,
    cf_hbm, ci_hbm, order_hbm,
    pred, in_z,
    x, obs, legf, legi, filt, win, wout, cf, ci, order,
    fwd, inv, normed, out_a0, out_a1, in_r0, in_r1, spec, out_b, in_q, in_y, grad,
    slot_ref, slot_smem, gain1, gain2,
    load_sem, x_sem, fs_sem, fr_sem, bs_sem, br_sem, ys_sem, yr_sem, zs_sem, zr_sem, small_sem,
):
    members = lax.axis_size("member")
    devices = lax.axis_size("lat")
    me = lax.axis_index("lat")
    mine = lax.axis_index("member")
    rows, length, channels = x.shape
    degrees = legf.shape[1]
    parts = out_a0.shape[2]
    outs_a, ins_r = [out_a0, out_a1], [in_r0, in_r1]
    slots = parts // 2
    block = length // members
    stride = 1

    def lat_peer(step):
        return (me + stride * step) % devices

    x_loads = [
        pltpu.make_async_copy(x_hbm.at[0, row], x.at[row], x_sem.at[row]) for row in range(rows)
    ]
    sources = [cf_hbm, ci_hbm, order_hbm, legf_hbm, legi_hbm, filt_hbm, win_hbm, wout_hbm]
    places = [cf, ci, order, legf, legi, filt, win, wout]
    loads = [
        pltpu.make_async_copy(source, place, load_sem.at[index])
        for index, (source, place) in enumerate(zip(sources, places))
    ]
    obs_load = pltpu.make_async_copy(
        obs_hbm.at[:, pl.ds(pl.multiple_of(mine * block, block), block), :],
        obs,
        load_sem.at[len(loads)],
    )
    small = [
        pltpu.make_async_copy(source, place, small_sem.at[index])
        for index, (source, place) in enumerate(
            [(slot_hbm, slot_ref), (gain1_hbm, gain1), (gain2_hbm, gain2), (slot_hbm, slot_smem)]
        )
    ]
    for load in small:
        load.start()
    loads[0].start()
    for load in x_loads:
        load.start()
    for load in loads[1:]:
        load.start()
    obs_load.start()

    barrier = pltpu.get_barrier_semaphore()

    def greet(step, carry):
        pl.semaphore_signal(barrier, inc=1, device_id=(mine, lat_peer(step)), device_id_type=MESH)
        return carry

    lax.fori_loop(devices // 2, devices, greet, 0)
    lax.fori_loop(1, devices // 2, greet, 0)
    for step in range(1, members):
        pl.semaphore_signal(
            barrier, inc=1, device_id=((mine + step) % members, me), device_id_type=MESH
        )

    for load in small:
        load.wait()
    spread = (degrees, 2 * degrees)
    gap = lax.broadcasted_iota(jnp.int32, spread, 1) - 2 * lax.broadcasted_iota(jnp.int32, spread, 0)
    twice = jnp.where((gap == 0) | (gap == 1), 2.0, 0.0).astype(BF16)
    waves = jnp.broadcast_to(slot_ref[...].astype(F32)[None, :], (8, degrees)).astype(BF16)
    columns = dot(waves, twice)[0:1].astype(jnp.int32)
    square = (2 * degrees, 2 * degrees)
    columns = columns + lax.broadcasted_iota(jnp.int32, (1, 2 * degrees), 1) % 2
    picked = jnp.where(lax.broadcasted_iota(jnp.int32, square, 0) == columns, 1.0, 0.0).astype(BF16)
    loads[0].wait()
    fwd[...] = lax.dot_general(
        picked, cf[...], (((0,), (0,)), ((), ())), preferred_element_type=F32
    ).astype(BF16)

    first = first_lanes(channels)
    chunks = [(0, first), (first, channels - first)]

    def norm_rows(row, carry):
        def norm_tile(tile, inner):
            at = pl.ds(pl.multiple_of(tile * wide, wide), wide)
            normed[row, at, :] = layer_norm(x[row, at, :].astype(F32), gain1[...][None, :]).astype(BF16)
            return inner

        return lax.fori_loop(0, length // wide, norm_tile, carry)

    wide = min(256, length)

    pair = rows // 2
    steps = [(0, pair, 0), (pair, pair, 0), (0, rows, 1)]
    for start, count, part in steps:
        lane, width = chunks[part]
        lanes, these = pl.ds(lane, width), pl.ds(start, count)
        out_a, in_r = outs_a[part], ins_r[part]
        if part == 0:
            for row in range(start, start + count):
                x_loads[row].wait()
            lax.fori_loop(start, start + count, norm_rows, 0)

        def analyse(row, carry):
            found = dot(fwd[...], normed[row, :, lanes]).astype(BF16)
            out_a[:, row] = found.reshape(devices, parts, width)
            return carry

        lax.fori_loop(start, start + count, analyse, 0)
        if start == 0 and part == 0:
            pl.semaphore_wait(barrier, devices - 1 + members - 1)

        def send(step, carry):
            peer = lat_peer(step)
            pltpu.make_async_remote_copy(
                src_ref=out_a.at[peer, these],
                dst_ref=in_r.at[me, these],
                send_sem=fs_sem.at[part],
                recv_sem=fr_sem.at[part],
                device_id=(mine, peer),
                device_id_type=MESH,
            ).start()
            return carry

        lax.fori_loop(1, devices, send, 0)
    for part in range(2):
        ins_r[part][me] = outs_a[part][me]

    loads[1].wait()
    inv[...] = dot(ci[...], picked).astype(BF16)
    for load in loads[2:]:
        load.wait()
    for slot in range(slots):
        local = slot_smem[me * slots + slot]
        level = lax.broadcasted_iota(jnp.int32, (degrees, degrees), 0)
        kept = legf[slot].astype(F32)
        legf[slot] = jnp.where(level >= local, kept, 0.0).astype(BF16)

    group = order.shape[0] // (rows * parts)
    points = group * rows

    def send_back(row, lanes):
        def send(step, carry):
            peer = lat_peer(step)
            pltpu.make_async_remote_copy(
                src_ref=out_b.at[peer, row, :, lanes],
                dst_ref=in_q.at[row, me, :, lanes],
                send_sem=bs_sem.at[row],
                recv_sem=br_sem.at[row],
                device_id=(mine, peer),
                device_id_type=MESH,
            ).start()
            return carry

        lax.fori_loop(1, devices, send, 0)

    for part, (lane, width) in enumerate(chunks):
        lanes = pl.ds(lane, width)
        in_r = ins_r[part]
        everything = in_r.at[pl.ds(0, devices - 1)]
        pltpu.make_async_copy(everything, everything, fr_sem.at[part]).wait()

        def gather(index, carry):
            taken = in_r[pl.ds(index * group, group)].reshape(points * parts, width)
            moved = dot(order[...], taken).astype(BF16)
            at = pl.ds(pl.multiple_of(index * points, points), points)
            spec[:, at, lanes] = moved.reshape(parts, points, width)
            return carry

        lax.fori_loop(0, devices // group, gather, 0)

        def transform(slot, carry):
            real = dot(legf[slot], spec[2 * slot, :, lanes])
            imag = dot(legf[slot], spec[2 * slot + 1, :, lanes])
            filt_real, filt_imag = filt[0, :, lanes], filt[1, :, lanes]
            new_real = (real * filt_real - imag * filt_imag).astype(BF16)
            new_imag = (real * filt_imag + imag * filt_real).astype(BF16)
            spec[2 * slot, :, lanes] = dot(legi[slot], new_real).astype(BF16)
            spec[2 * slot + 1, :, lanes] = dot(legi[slot], new_imag).astype(BF16)
            return carry

        lax.fori_loop(0, slots, transform, 0)

        def scatter(index, carry):
            at = pl.ds(pl.multiple_of(index * points, points), points)
            taken = spec[:, at, lanes].reshape(points * parts, width)
            moved = lax.dot_general(
                order[...], taken, (((0,), (0,)), ((), ())), preferred_element_type=F32
            ).astype(BF16)
            out_b[pl.ds(index * group, group), :, :, lanes] = moved.reshape(group, rows, parts, width)
            return carry

        lax.fori_loop(0, devices // group, scatter, 0)
        send_back(0, lanes)

    everywhere = pl.ds(0, channels)

    def send_rest(row, carry):
        send_back(row, everywhere)
        return carry

    lax.fori_loop(1, rows, send_rest, 0)
    for row in range(rows):
        in_q[row, me] = out_b[me, row]
    obs_load.wait()

    halves = in_y.shape[1]
    piece = block // halves
    thin = min(32, piece)

    def spans(half):
        return [
            pl.ds(pl.multiple_of(index * block + half * piece, piece), piece)
            for index in range(members)
        ]

    def predict(row, half):
        waves = in_q[row].reshape(devices * parts, channels)
        table = jnp.concatenate([inv[at, :] for at in spans(half)], 0)
        before = jnp.concatenate([x[row, at, :] for at in spans(half)], 0)
        after = before.astype(F32) + dot(table, waves)
        second = layer_norm(after, gain2[...][None, :]).astype(BF16)
        hidden = jax.nn.gelu(dot(second, win[...])).astype(BF16)
        result = (after + dot(hidden, wout[...])).astype(BF16)
        for index, at in enumerate(spans(half)):
            pred[row, at, :] = result[index * piece : (index + 1) * piece]
        for step in range(1, members):
            peer = (mine + step) % members
            pltpu.make_async_remote_copy(
                src_ref=pred.at[row, pl.ds(pl.multiple_of(peer * block + half * piece, piece), piece), :],
                dst_ref=in_y.at[row, half, mine],
                send_sem=ys_sem.at[row * halves + half],
                recv_sem=yr_sem.at[row * halves + half],
                device_id=(peer, me),
                device_id_type=MESH,
            ).start()

    def score(row, half):
        arrived = in_y.at[row, half, pl.ds(0, members - 1)]
        pltpu.make_async_copy(arrived, arrived, yr_sem.at[row * halves + half]).wait()
        own = pl.ds(pl.multiple_of(mine * block + half * piece, piece), piece)
        in_y[row, half, mine] = pred[row, own, :]

        def score_rows(tile, carry):
            at = pl.ds(pl.multiple_of(tile * thin, thin), thin)
            fields = [in_y[row, half, index, at, :].astype(F32) for index in range(members)]
            here = pl.ds(pl.multiple_of(half * piece + tile * thin, thin), thin)
            target = obs[row, here, :].astype(F32)
            slopes = []
            for index in range(members):
                gap = fields[index] - target
                slopes.append(gap * inverse_distance(gap))
            for one in range(members):
                for two in range(one + 1, members):
                    gap = fields[one] - fields[two]
                    pull = gap * (inverse_distance(gap) * (1.0 / (members - 1)))
                    slopes[one] = slopes[one] - pull
                    slopes[two] = slopes[two] + pull
            for index in range(members):
                grad[row, half, index, at, :] = slopes[index].astype(BF16)
            return carry

        lax.fori_loop(0, piece // thin, score_rows, 0)
        there = pl.ds(pl.multiple_of(half * piece, piece), piece)
        for step in range(1, members):
            peer = (mine + step) % members
            pltpu.make_async_remote_copy(
                src_ref=grad.at[row, half, peer],
                dst_ref=in_z.at[row, mine, there, :],
                send_sem=zs_sem.at[row * halves + half],
                recv_sem=zr_sem.at[row * halves + half],
                device_id=(peer, me),
                device_id_type=MESH,
            ).start()
        in_z[row, mine, there, :] = grad[row, half, mine]

    def finish(row, carry):
        arrived = in_q.at[row, pl.ds(0, devices - 1)]
        pltpu.make_async_copy(arrived, arrived, br_sem.at[row]).wait()

        def predict_half(half, inner):
            predict(row, half)
            return inner

        def score_half(half, inner):
            score(row, half)
            return inner

        lax.fori_loop(0, halves, predict_half, 0)
        lax.fori_loop(0, halves, score_half, 0)
        return carry

    lax.fori_loop(0, rows, finish, 0)

    def deliver(index, carry):
        arrived = in_y.at[0, 0, pl.ds(0, members - 1)]
        pltpu.make_async_copy(arrived, arrived, zr_sem.at[index]).wait()
        pltpu.make_async_copy(arrived, arrived, ys_sem.at[index]).wait()
        pltpu.make_async_copy(arrived, arrived, zs_sem.at[index]).wait()
        return carry

    lax.fori_loop(0, rows * halves, deliver, 0)

    for part, (lane, width) in enumerate(chunks):
        sent = outs_a[part].at[pl.ds(0, devices - 1)]
        pltpu.make_async_copy(sent, sent, fs_sem.at[part]).wait()

    def drain(row, carry):
        sent = in_q.at[row, pl.ds(0, devices - 1)]
        pltpu.make_async_copy(sent, sent, bs_sem.at[row]).wait()
        return carry

    lax.fori_loop(0, rows, drain, 0)


def store(pred, slope, pred_out, slope_out, sem):
    copies = [
        pltpu.make_async_copy(pred, pred_out.at[0], sem.at[0]),
        pltpu.make_async_copy(slope, slope_out.at[0], sem.at[1]),
    ]
    for copy in copies:
        copy.start()
    for copy in copies:
        copy.wait()


def local(
    ensemble_starting_fields, observed, wave_of_slot, leg_forward, leg_inverse, spec_filter,
    gain_first, gain_second, weight_in, weight_out,
):
    _, rows, length, channels = ensemble_starting_fields.shape
    waves = wave_of_slot.shape[0]
    slots, degrees, lats = leg_forward.shape
    hidden = weight_in.shape[1]
    devices = lax.axis_size("lat")
    members = lax.axis_size("member")
    block = length // members
    parts = 2 * slots
    halves = 4
    first = first_lanes(channels)
    forward, inverse = tables(waves, length)
    group = min(8, devices)
    order = group_order(group * rows, parts)
    whole = pl.BlockSpec(memory_space=pltpu.HBM)
    near = pl.BlockSpec(memory_space=pltpu.VMEM)
    sems = pltpu.SemaphoreType.DMA
    operands = [
        ensemble_starting_fields, observed, wave_of_slot, leg_forward, leg_inverse, spec_filter,
        gain_first, gain_second, weight_in, weight_out, forward, inverse, order,
    ]
    operands = [pltpu.with_memory_space_constraint(operand, pltpu.HBM) for operand in operands]
    pred, slope = pl.pallas_call(
        kernel,
        out_shape=(
            pltpu.VMEM((rows, length, channels), BF16),
            pltpu.VMEM((rows, members, block, channels), BF16),
        ),
        in_specs=[whole] * 13,
        out_specs=(near, near),
        scratch_shapes=[
            pltpu.VMEM((rows, length, channels), BF16),
            pltpu.VMEM((rows, block, channels), BF16),
            pltpu.VMEM((slots, degrees, lats), BF16),
            pltpu.VMEM((slots, lats, degrees), BF16),
            pltpu.VMEM((2, degrees, channels), F32),
            pltpu.VMEM((channels, hidden), BF16),
            pltpu.VMEM((hidden, channels), BF16),
            pltpu.VMEM((2 * waves, length), BF16),
            pltpu.VMEM((length, 2 * waves), BF16),
            pltpu.VMEM(order.shape, BF16),
            pltpu.VMEM((2 * waves, length), BF16),
            pltpu.VMEM((length, 2 * waves), BF16),
            pltpu.VMEM((rows, length, channels), BF16),
            pltpu.VMEM((devices, rows, parts, first), BF16),
            pltpu.VMEM((devices, rows, parts, channels - first), BF16),
            pltpu.VMEM((devices, rows, parts, first), BF16),
            pltpu.VMEM((devices, rows, parts, channels - first), BF16),
            pltpu.VMEM((parts, lats, channels), BF16),
            pltpu.VMEM((devices, rows, parts, channels), BF16),
            pltpu.VMEM((rows, devices, parts, channels), BF16),
            pltpu.VMEM((rows, halves, members, block // halves, channels), BF16),
            pltpu.VMEM((rows, halves, members, block // halves, channels), BF16),
            pltpu.VMEM((waves,), jnp.int32),
            pltpu.SMEM((waves,), jnp.int32),
            pltpu.VMEM((channels,), F32),
            pltpu.VMEM((channels,), F32),
            sems((9,)),
            sems((rows,)),
            sems((2,)),
            sems((2,)),
            sems((rows,)),
            sems((rows,)),
            sems((rows * halves,)),
            sems((rows * halves,)),
            sems((rows * halves,)),
            sems((rows * halves,)),
            sems((4,)),
        ],
        compiler_params=pltpu.CompilerParams(
            collective_id=0, has_side_effects=True, vmem_limit_bytes=48 * 1024 * 1024
        ),
    )(*operands)
    results = [pred, slope.reshape(rows, length, channels)]
    results = [pltpu.with_memory_space_constraint(result, pltpu.VMEM) for result in results]
    shape = jax.ShapeDtypeStruct((1, rows, length, channels), BF16)
    pred, slope = pl.pallas_call(
        store,
        out_shape=(shape, shape),
        in_specs=[near, near],
        out_specs=(whole, whole),
        scratch_shapes=[sems((2,))],
    )(*results)
    return (pred, slope)


def solution(mesh):
    in_specs = (
        P("member", "lat", None, None),
        P("lat", None, None),
        P(),
        P("lat", None, None),
        P("lat", None, None),
        P(),
        P(),
        P(),
        P(),
        P(),
    )
    out_specs = (P("member", "lat", None, None), P("member", "lat", None, None))
    return jax.shard_map(local, mesh=mesh, in_specs=in_specs, out_specs=out_specs, check_vma=False)
```

```python
import functools
import math

import jax
import jax.numpy as jnp
import numpy as np
from jax import lax
from jax.experimental import pallas as pl
from jax.experimental.pallas import tpu as pltpu
from jax.sharding import PartitionSpec as P

EPS_NORM = 1e-05
EPS_DIST = 1e-06
MESH = pl.DeviceIdType.MESH
F32 = jnp.float32
BF16 = jnp.bfloat16


def tables(waves, length):
    m = np.arange(waves)[:, None]
    j = np.arange(length)[None, :]
    angle = (m * j % length) * (2.0 * math.pi / length)
    cosine, sine = np.cos(angle), np.sin(angle)
    forward = np.stack([cosine / length, -sine / length], 1).reshape(2 * waves, length)
    weight = np.where(m == 0, 1.0, 2.0)
    inverse = np.stack([weight * cosine, -weight * sine], 1).reshape(2 * waves, length).T
    return jnp.asarray(forward, BF16), jnp.asarray(inverse, BF16)


def group_order(points, parts):
    rows = np.arange(points * parts)
    part, point = rows // points, rows % points
    order = np.zeros((points * parts, points * parts), np.float32)
    order[rows, point * parts + part] = 1.0
    return jnp.asarray(order, BF16)


def layer_norm(values, scales):
    average = jnp.mean(values, -1, keepdims=True)
    centred = values - average
    spread = jnp.mean(centred * centred, -1, keepdims=True)
    return centred * lax.rsqrt(spread + EPS_NORM) * scales


def inverse_distance(difference):
    return lax.rsqrt(jnp.mean(jnp.square(difference), -1, keepdims=True) + EPS_DIST)


def first_lanes(channels):
    return 2 * channels // 3 // 128 * 128


def dot(a, b):
    return jnp.dot(a, b, preferred_element_type=F32)


def kernel(
    x_hbm, obs_hbm, slot_hbm, legf_hbm, legi_hbm, filt_hbm, gain1_hbm, gain2_hbm, win_hbm, wout_hbm,
    cf_hbm, ci_hbm, order_hbm,
    pred, in_z,
    x, obs, legf, legi, filt, win, wout, cf, ci, order,
    fwd, inv, normed, out_a0, out_a1, in_r0, in_r1, spec, out_b, in_q, in_y, grad,
    slot_ref, slot_smem, gain1, gain2,
    load_sem, x_sem, fs_sem, fr_sem, bs_sem, br_sem, ys_sem, yr_sem, zs_sem, zr_sem, small_sem,
):
    members = lax.axis_size("member")
    devices = lax.axis_size("lat")
    me = lax.axis_index("lat")
    mine = lax.axis_index("member")
    rows, length, channels = x.shape
    degrees = legf.shape[1]
    parts = out_a0.shape[2]
    outs_a, ins_r = [out_a0, out_a1], [in_r0, in_r1]
    slots = parts // 2
    block = length // members
    stride = 1

    def lat_peer(step):
        return (me + stride * step) % devices

    x_loads = [
        pltpu.make_async_copy(x_hbm.at[0, row], x.at[row], x_sem.at[row]) for row in range(rows)
    ]
    sources = [cf_hbm, ci_hbm, order_hbm, legf_hbm, legi_hbm, filt_hbm, win_hbm, wout_hbm]
    places = [cf, ci, order, legf, legi, filt, win, wout]
    loads = [
        pltpu.make_async_copy(source, place, load_sem.at[index])
        for index, (source, place) in enumerate(zip(sources, places))
    ]
    obs_load = pltpu.make_async_copy(
        obs_hbm.at[:, pl.ds(pl.multiple_of(mine * block, block), block), :],
        obs,
        load_sem.at[len(loads)],
    )
    small = [
        pltpu.make_async_copy(source, place, small_sem.at[index])
        for index, (source, place) in enumerate(
            [(slot_hbm, slot_ref), (gain1_hbm, gain1), (gain2_hbm, gain2), (slot_hbm, slot_smem)]
        )
    ]
    for load in small:
        load.start()
    loads[0].start()
    for load in x_loads:
        load.start()
    for load in loads[1:]:
        load.start()
    obs_load.start()

    barrier = pltpu.get_barrier_semaphore()

    def greet(step, carry):
        pl.semaphore_signal(barrier, inc=1, device_id=(mine, lat_peer(step)), device_id_type=MESH)
        return carry

    lax.fori_loop(devices // 2, devices, greet, 0)
    lax.fori_loop(1, devices // 2, greet, 0)
    for step in range(1, members):
        pl.semaphore_signal(
            barrier, inc=1, device_id=((mine + step) % members, me), device_id_type=MESH
        )

    for load in small:
        load.wait()
    spread = (degrees, 2 * degrees)
    gap = lax.broadcasted_iota(jnp.int32, spread, 1) - 2 * lax.broadcasted_iota(jnp.int32, spread, 0)
    twice = jnp.where((gap == 0) | (gap == 1), 2.0, 0.0).astype(BF16)
    waves = jnp.broadcast_to(slot_ref[...].astype(F32)[None, :], (8, degrees)).astype(BF16)
    columns = dot(waves, twice)[0:1].astype(jnp.int32)
    square = (2 * degrees, 2 * degrees)
    columns = columns + lax.broadcasted_iota(jnp.int32, (1, 2 * degrees), 1) % 2
    picked = jnp.where(lax.broadcasted_iota(jnp.int32, square, 0) == columns, 1.0, 0.0).astype(BF16)
    loads[0].wait()
    fwd[...] = lax.dot_general(
        picked, cf[...], (((0,), (0,)), ((), ())), preferred_element_type=F32
    ).astype(BF16)

    first = first_lanes(channels)
    chunks = [(0, first), (first, channels - first)]

    def norm_rows(row, carry):
        def norm_tile(tile, inner):
            at = pl.ds(pl.multiple_of(tile * wide, wide), wide)
            normed[row, at, :] = layer_norm(x[row, at, :].astype(F32), gain1[...][None, :]).astype(BF16)
            return inner

        return lax.fori_loop(0, length // wide, norm_tile, carry)

    wide = min(256, length)

    pair = rows // 2
    steps = [(0, pair, 0), (pair, pair, 0), (0, rows, 1)]
    for start, count, part in steps:
        lane, width = chunks[part]
        lanes, these = pl.ds(lane, width), pl.ds(start, count)
        out_a, in_r = outs_a[part], ins_r[part]
        if part == 0:
            for row in range(start, start + count):
                x_loads[row].wait()
            lax.fori_loop(start, start + count, norm_rows, 0)

        def analyse(row, carry):
            found = dot(fwd[...], normed[row, :, lanes]).astype(BF16)
            out_a[:, row] = found.reshape(devices, parts, width)
            return carry

        lax.fori_loop(start, start + count, analyse, 0)
        if start == 0 and part == 0:
            pl.semaphore_wait(barrier, devices - 1 + members - 1)

        def send(step, carry):
            peer = lat_peer(step)
            pltpu.make_async_remote_copy(
                src_ref=out_a.at[peer, these],
                dst_ref=in_r.at[me, these],
                send_sem=fs_sem.at[part],
                recv_sem=fr_sem.at[part],
                device_id=(mine, peer),
                device_id_type=MESH,
            ).start()
            return carry

        lax.fori_loop(1, devices, send, 0)
    for part in range(2):
        ins_r[part][me] = outs_a[part][me]

    loads[1].wait()
    inv[...] = dot(ci[...], picked).astype(BF16)
    for load in loads[2:]:
        load.wait()
    for slot in range(slots):
        local = slot_smem[me * slots + slot]
        level = lax.broadcasted_iota(jnp.int32, (degrees, degrees), 0)
        kept = legf[slot].astype(F32)
        legf[slot] = jnp.where(level >= local, kept, 0.0).astype(BF16)

    group = order.shape[0] // (rows * parts)
    points = group * rows

    def send_back(row, lanes):
        def send(step, carry):
            peer = lat_peer(step)
            pltpu.make_async_remote_copy(
                src_ref=out_b.at[peer, row, :, lanes],
                dst_ref=in_q.at[row, me, :, lanes],
                send_sem=bs_sem.at[row],
                recv_sem=br_sem.at[row],
                device_id=(mine, peer),
                device_id_type=MESH,
            ).start()
            return carry

        lax.fori_loop(1, devices, send, 0)

    for part, (lane, width) in enumerate(chunks):
        lanes = pl.ds(lane, width)
        in_r = ins_r[part]
        everything = in_r.at[pl.ds(0, devices - 1)]
        pltpu.make_async_copy(everything, everything, fr_sem.at[part]).wait()

        def gather(index, carry):
            taken = in_r[pl.ds(index * group, group)].reshape(points * parts, width)
            moved = dot(order[...], taken).astype(BF16)
            at = pl.ds(pl.multiple_of(index * points, points), points)
            spec[:, at, lanes] = moved.reshape(parts, points, width)
            return carry

        lax.fori_loop(0, devices // group, gather, 0)

        def transform(slot, carry):
            real = dot(legf[slot], spec[2 * slot, :, lanes])
            imag = dot(legf[slot], spec[2 * slot + 1, :, lanes])
            filt_real, filt_imag = filt[0, :, lanes], filt[1, :, lanes]
            new_real = (real * filt_real - imag * filt_imag).astype(BF16)
            new_imag = (real * filt_imag + imag * filt_real).astype(BF16)
            spec[2 * slot, :, lanes] = dot(legi[slot], new_real).astype(BF16)
            spec[2 * slot + 1, :, lanes] = dot(legi[slot], new_imag).astype(BF16)
            return carry

        lax.fori_loop(0, slots, transform, 0)

        def scatter(index, carry):
            at = pl.ds(pl.multiple_of(index * points, points), points)
            taken = spec[:, at, lanes].reshape(points * parts, width)
            moved = lax.dot_general(
                order[...], taken, (((0,), (0,)), ((), ())), preferred_element_type=F32
            ).astype(BF16)
            out_b[pl.ds(index * group, group), :, :, lanes] = moved.reshape(group, rows, parts, width)
            return carry

        lax.fori_loop(0, devices // group, scatter, 0)
        send_back(0, lanes)

    everywhere = pl.ds(0, channels)

    def send_rest(row, carry):
        send_back(row, everywhere)
        return carry

    lax.fori_loop(1, rows, send_rest, 0)
    for row in range(rows):
        in_q[row, me] = out_b[me, row]
    obs_load.wait()

    halves = in_y.shape[1]
    piece = block // halves
    thin = min(32, piece)

    def spans(half):
        return [
            pl.ds(pl.multiple_of(index * block + half * piece, piece), piece)
            for index in range(members)
        ]

    def predict(row, half):
        waves = in_q[row].reshape(devices * parts, channels)
        table = jnp.concatenate([inv[at, :] for at in spans(half)], 0)
        before = jnp.concatenate([x[row, at, :] for at in spans(half)], 0)
        after = before.astype(F32) + dot(table, waves)
        second = layer_norm(after, gain2[...][None, :]).astype(BF16)
        hidden = jax.nn.gelu(dot(second, win[...])).astype(BF16)
        result = (after + dot(hidden, wout[...])).astype(BF16)
        for index, at in enumerate(spans(half)):
            pred[row, at, :] = result[index * piece : (index + 1) * piece]
        for step in range(1, members):
            peer = (mine + step) % members
            pltpu.make_async_remote_copy(
                src_ref=pred.at[row, pl.ds(pl.multiple_of(peer * block + half * piece, piece), piece), :],
                dst_ref=in_y.at[row, half, mine],
                send_sem=ys_sem.at[row * halves + half],
                recv_sem=yr_sem.at[row * halves + half],
                device_id=(peer, me),
                device_id_type=MESH,
            ).start()

    def score(row, half):
        arrived = in_y.at[row, half, pl.ds(0, members - 1)]
        pltpu.make_async_copy(arrived, arrived, yr_sem.at[row * halves + half]).wait()
        own = pl.ds(pl.multiple_of(mine * block + half * piece, piece), piece)
        in_y[row, half, mine] = pred[row, own, :]

        def score_rows(tile, carry):
            at = pl.ds(pl.multiple_of(tile * thin, thin), thin)
            fields = [in_y[row, half, index, at, :].astype(F32) for index in range(members)]
            here = pl.ds(pl.multiple_of(half * piece + tile * thin, thin), thin)
            target = obs[row, here, :].astype(F32)
            slopes = []
            for index in range(members):
                gap = fields[index] - target
                slopes.append(gap * inverse_distance(gap))
            for one in range(members):
                for two in range(one + 1, members):
                    gap = fields[one] - fields[two]
                    pull = gap * (inverse_distance(gap) * (1.0 / (members - 1)))
                    slopes[one] = slopes[one] - pull
                    slopes[two] = slopes[two] + pull
            for index in range(members):
                grad[row, half, index, at, :] = slopes[index].astype(BF16)
            return carry

        lax.fori_loop(0, piece // thin, score_rows, 0)
        there = pl.ds(pl.multiple_of(half * piece, piece), piece)
        for step in range(1, members):
            peer = (mine + step) % members
            pltpu.make_async_remote_copy(
                src_ref=grad.at[row, half, peer],
                dst_ref=in_z.at[row, mine, there, :],
                send_sem=zs_sem.at[row * halves + half],
                recv_sem=zr_sem.at[row * halves + half],
                device_id=(peer, me),
                device_id_type=MESH,
            ).start()
        in_z[row, mine, there, :] = grad[row, half, mine]

    def finish(row, carry):
        arrived = in_q.at[row, pl.ds(0, devices - 1)]
        pltpu.make_async_copy(arrived, arrived, br_sem.at[row]).wait()

        def predict_half(half, inner):
            predict(row, half)
            return inner

        def score_half(half, inner):
            score(row, half)
            return inner

        lax.fori_loop(0, halves, predict_half, 0)
        lax.fori_loop(0, halves, score_half, 0)
        return carry

    lax.fori_loop(0, rows, finish, 0)

    def deliver(index, carry):
        arrived = in_y.at[0, 0, pl.ds(0, members - 1)]
        pltpu.make_async_copy(arrived, arrived, zr_sem.at[index]).wait()
        pltpu.make_async_copy(arrived, arrived, ys_sem.at[index]).wait()
        pltpu.make_async_copy(arrived, arrived, zs_sem.at[index]).wait()
        return carry

    lax.fori_loop(0, rows * halves, deliver, 0)

    for part, (lane, width) in enumerate(chunks):
        sent = outs_a[part].at[pl.ds(0, devices - 1)]
        pltpu.make_async_copy(sent, sent, fs_sem.at[part]).wait()

    def drain(row, carry):
        sent = in_q.at[row, pl.ds(0, devices - 1)]
        pltpu.make_async_copy(sent, sent, bs_sem.at[row]).wait()
        return carry

    lax.fori_loop(0, rows, drain, 0)


def store(pred, slope, pred_out, slope_out, sem):
    copies = [
        pltpu.make_async_copy(pred, pred_out.at[0], sem.at[0]),
        pltpu.make_async_copy(slope, slope_out.at[0], sem.at[1]),
    ]
    for copy in copies:
        copy.start()
    for copy in copies:
        copy.wait()


def local(
    ensemble_starting_fields, observed, wave_of_slot, leg_forward, leg_inverse, spec_filter,
    gain_first, gain_second, weight_in, weight_out,
):
    _, rows, length, channels = ensemble_starting_fields.shape
    waves = wave_of_slot.shape[0]
    slots, degrees, lats = leg_forward.shape
    hidden = weight_in.shape[1]
    devices = lax.axis_size("lat")
    members = lax.axis_size("member")
    block = length // members
    parts = 2 * slots
    halves = 8
    first = first_lanes(channels)
    forward, inverse = tables(waves, length)
    group = min(8, devices)
    order = group_order(group * rows, parts)
    whole = pl.BlockSpec(memory_space=pltpu.HBM)
    near = pl.BlockSpec(memory_space=pltpu.VMEM)
    sems = pltpu.SemaphoreType.DMA
    operands = [
        ensemble_starting_fields, observed, wave_of_slot, leg_forward, leg_inverse, spec_filter,
        gain_first, gain_second, weight_in, weight_out, forward, inverse, order,
    ]
    operands = [pltpu.with_memory_space_constraint(operand, pltpu.HBM) for operand in operands]
    pred, slope = pl.pallas_call(
        kernel,
        out_shape=(
            pltpu.VMEM((rows, length, channels), BF16),
            pltpu.VMEM((rows, members, block, channels), BF16),
        ),
        in_specs=[whole] * 13,
        out_specs=(near, near),
        scratch_shapes=[
            pltpu.VMEM((rows, length, channels), BF16),
            pltpu.VMEM((rows, block, channels), BF16),
            pltpu.VMEM((slots, degrees, lats), BF16),
            pltpu.VMEM((slots, lats, degrees), BF16),
            pltpu.VMEM((2, degrees, channels), F32),
            pltpu.VMEM((channels, hidden), BF16),
            pltpu.VMEM((hidden, channels), BF16),
            pltpu.VMEM((2 * waves, length), BF16),
            pltpu.VMEM((length, 2 * waves), BF16),
            pltpu.VMEM(order.shape, BF16),
            pltpu.VMEM((2 * waves, length), BF16),
            pltpu.VMEM((length, 2 * waves), BF16),
            pltpu.VMEM((rows, length, channels), BF16),
            pltpu.VMEM((devices, rows, parts, first), BF16),
            pltpu.VMEM((devices, rows, parts, channels - first), BF16),
            pltpu.VMEM((devices, rows, parts, first), BF16),
            pltpu.VMEM((devices, rows, parts, channels - first), BF16),
            pltpu.VMEM((parts, lats, channels), BF16),
            pltpu.VMEM((devices, rows, parts, channels), BF16),
            pltpu.VMEM((rows, devices, parts, channels), BF16),
            pltpu.VMEM((rows, halves, members, block // halves, channels), BF16),
            pltpu.VMEM((rows, halves, members, block // halves, channels), BF16),
            pltpu.VMEM((waves,), jnp.int32),
            pltpu.SMEM((waves,), jnp.int32),
            pltpu.VMEM((channels,), F32),
            pltpu.VMEM((channels,), F32),
            sems((9,)),
            sems((rows,)),
            sems((2,)),
            sems((2,)),
            sems((rows,)),
            sems((rows,)),
            sems((rows * halves,)),
            sems((rows * halves,)),
            sems((rows * halves,)),
            sems((rows * halves,)),
            sems((4,)),
        ],
        compiler_params=pltpu.CompilerParams(
            collective_id=0, has_side_effects=True, vmem_limit_bytes=48 * 1024 * 1024
        ),
    )(*operands)
    results = [pred, slope.reshape(rows, length, channels)]
    results = [pltpu.with_memory_space_constraint(result, pltpu.VMEM) for result in results]
    shape = jax.ShapeDtypeStruct((1, rows, length, channels), BF16)
    pred, slope = pl.pallas_call(
        store,
        out_shape=(shape, shape),
        in_specs=[near, near],
        out_specs=(whole, whole),
        scratch_shapes=[sems((2,))],
    )(*results)
    return (pred, slope)


def solution(mesh):
    in_specs = (
        P("member", "lat", None, None),
        P("lat", None, None),
        P(),
        P("lat", None, None),
        P("lat", None, None),
        P(),
        P(),
        P(),
        P(),
        P(),
    )
    out_specs = (P("member", "lat", None, None), P("member", "lat", None, None))
    return jax.shard_map(local, mesh=mesh, in_specs=in_specs, out_specs=out_specs, check_vma=False)
```
